16 devices in a mesh: dp: 2 (over y, z), tp: 8 (over x, core).
Axes of the slice: x: 4, y: 2, z: 1, core: 2. Of those that a mesh axis runs over, the one named last changes fastest.
The devices are a block of a 4x4x8 slice.
Arguments:
- k_cache: bfloat16 [8, 32, 4096, 128], P('dp', None, 'tp'), parts along dimension 0
- v_cache: bfloat16 [8, 32, 4096, 128], P('dp', None, 'tp'), parts along dimension 0
- prompt_len: int32 [8], P('dp'), parts along dimension 0
- x_steps: bfloat16 [64, 8, 4096], P(None, 'dp'), parts along dimension 1
- w_norm: bfloat16 [4096], replicated
- w_q: bfloat16 [4096, 4096], P(None, 'tp')
- w_k: bfloat16 [4096, 4096], P(None, 'tp')
- w_v: bfloat16 [4096, 4096], P(None, 'tp')
- w_o: bfloat16 [4096, 4096], P('tp')
Outputs:
- output 1: bfloat16 [64, 8, 4096], P(None, 'dp'), parts along dimension 1
- output 2: bfloat16 [8, 32, 4160, 128], P('dp', 'tp'), parts along dimension 0
- output 3: bfloat16 [8, 32, 4160, 128], P('dp', 'tp'), parts along dimension 0
There are 2 independent parts. The reference program is written for one: setup_inputs(seed, part) draws one part's arguments, and reference() takes and returns one part's arrays. A program takes and returns all parts, laid end to end along the dimension named above; an argument that names none is the same for every part.
All inputs are finite; a program needn't handle non-finite values.
Results may differ from the reference program's by a relative error of at most 0.0174102.
Values are sent between devices in bfloat16 or wider.
A program may use at most 768 MiB of HBM per device.

```python
import jax
import jax.numpy as jnp
from jax import lax

MODEL_DIM = 4096
NUM_HEADS = 32
HEAD_DIM = 128
BATCH_ROWS = 4
SEQ_LEN = 4096
DECODE_STEPS = 64


def rotate(values, positions):
    half_dim = HEAD_DIM // 2
    inv_freq = 10000.0 ** (-2.0 * jnp.arange(half_dim, dtype=jnp.float32) / HEAD_DIM)
    angles = positions.astype(jnp.float32)[..., None] * inv_freq
    cos_part = jnp.cos(angles)
    sin_part = jnp.sin(angles)
    first_half = values[..., :half_dim]
    second_half = values[..., half_dim:]
    return jnp.concatenate([first_half * cos_part - second_half * sin_part, second_half * cos_part + first_half * sin_part], axis=-1)


def setup_inputs(seed: int = 0, part: int = 0) -> dict:
    part_key = jax.random.fold_in(jax.random.key(seed), part)
    draw_keys = jax.random.split(part_key, 6)
    shared_keys = jax.random.split(jax.random.key(seed + 1), 5)
    proj_width = NUM_HEADS * HEAD_DIM
    cache_shape = (BATCH_ROWS, NUM_HEADS, SEQ_LEN, HEAD_DIM)
    k_cache = jax.random.normal(draw_keys[0], cache_shape, jnp.float32).astype(jnp.bfloat16)
    v_cache = jax.random.normal(draw_keys[1], cache_shape, jnp.float32).astype(jnp.bfloat16)
    half_len = SEQ_LEN // 2
    lengths = jax.random.randint(draw_keys[2], (BATCH_ROWS,), half_len, SEQ_LEN + 1)
    long_row = jax.random.randint(draw_keys[3], (), 0, BATCH_ROWS)
    short_row = (long_row + jax.random.randint(draw_keys[4], (), 1, BATCH_ROWS)) % BATCH_ROWS
    row_ids = jnp.arange(BATCH_ROWS)
    lengths = jnp.where(row_ids == long_row, SEQ_LEN, lengths)
    lengths = jnp.where(row_ids == short_row, half_len, lengths)
    x_steps = jax.random.normal(draw_keys[5], (DECODE_STEPS, BATCH_ROWS, MODEL_DIM), jnp.float32).astype(jnp.bfloat16)
    w_norm = (0.5 * jax.random.normal(shared_keys[0], (MODEL_DIM,), jnp.float32)).astype(jnp.bfloat16)
    in_scale = MODEL_DIM ** -0.5
    w_q = (in_scale * jax.random.normal(shared_keys[1], (MODEL_DIM, proj_width), jnp.float32)).astype(jnp.bfloat16)
    w_k = (in_scale * jax.random.normal(shared_keys[2], (MODEL_DIM, proj_width), jnp.float32)).astype(jnp.bfloat16)
    w_v = (in_scale * jax.random.normal(shared_keys[3], (MODEL_DIM, proj_width), jnp.float32)).astype(jnp.bfloat16)
    out_scale = (SEQ_LEN / (4.0 * proj_width)) ** 0.5
    w_o = (out_scale * jax.random.normal(shared_keys[4], (proj_width, MODEL_DIM), jnp.float32)).astype(jnp.bfloat16)
    return {"k_cache": k_cache, "v_cache": v_cache, "prompt_len": lengths.astype(jnp.int32), "x_steps": x_steps, "w_norm": w_norm, "w_q": w_q, "w_k": w_k, "w_v": w_v, "w_o": w_o}


def reference(k_cache, v_cache, prompt_len, x_steps, w_norm, w_q, w_k, w_v, w_o):
    out_len = SEQ_LEN + DECODE_STEPS
    q_scale = HEAD_DIM ** -0.5
    norm_gain = 1.0 + w_norm.astype(jnp.float32)
    zero_tail = jnp.zeros((BATCH_ROWS, NUM_HEADS, DECODE_STEPS, HEAD_DIM), jnp.float32)
    keys_init = jnp.concatenate([k_cache.astype(jnp.float32), zero_tail], axis=2)
    vals_init = jnp.concatenate([v_cache.astype(jnp.float32), zero_tail], axis=2)
    slot_ids = jnp.arange(out_len)

    def write_row(cache_row, new_row, start_slot):
        return lax.dynamic_update_slice(cache_row, new_row, (0, start_slot, 0))

    def project(normed, weight):
        proj_flat = jnp.dot(normed, weight, preferred_element_type=jnp.float32).astype(jnp.bfloat16)
        return proj_flat.reshape(BATCH_ROWS, NUM_HEADS, HEAD_DIM).astype(jnp.float32)

    def step(state_in, step_in):
        keys_all, vals_all = state_in
        x_step, step_idx = step_in
        residual = x_step.astype(jnp.float32)
        inv_rms = lax.rsqrt(jnp.mean(residual * residual, axis=-1, keepdims=True) + 1e-6)
        normed = (residual * inv_rms * norm_gain).astype(jnp.bfloat16)
        position = prompt_len + step_idx
        queries = (rotate(project(normed, w_q), position[:, None]) * q_scale).astype(jnp.bfloat16).astype(jnp.float32)
        key_new = rotate(project(normed, w_k), position[:, None]).astype(jnp.bfloat16).astype(jnp.float32)
        val_new = project(normed, w_v)
        keys_all = jax.vmap(write_row)(keys_all, key_new[:, :, None, :], position)
        vals_all = jax.vmap(write_row)(vals_all, val_new[:, :, None, :], position)
        scores = jnp.einsum("bhd,bhtd->bht", queries, keys_all)
        is_valid = (slot_ids[None, :] <= position[:, None])[:, None, :]
        scores = jnp.where(is_valid, scores, -jnp.inf)
        row_peak = jnp.max(scores, axis=-1, keepdims=True)
        exp_scores = jnp.exp(scores - row_peak)
        attn_probs = (exp_scores / jnp.sum(exp_scores, axis=-1, keepdims=True)).astype(jnp.bfloat16).astype(jnp.float32)
        heads_out = jnp.einsum("bht,bhtd->bhd", attn_probs, vals_all).astype(jnp.bfloat16)
        attn_part = jnp.dot(heads_out.reshape(BATCH_ROWS, NUM_HEADS * HEAD_DIM), w_o, preferred_element_type=jnp.float32)
        return (keys_all, vals_all), (residual + attn_part).astype(jnp.bfloat16)

    final_state, y_steps = lax.scan(step, (keys_init, vals_init), (x_steps, jnp.arange(DECODE_STEPS)))
    return y_steps, final_state[0].astype(jnp.bfloat16), final_state[1].astype(jnp.bfloat16)
```

```python
import functools

import jax
import jax.numpy as jnp
from jax import lax
from jax.experimental import pallas as pl
from jax.experimental.pallas import tpu as pltpu
from jax.sharding import PartitionSpec as P

ROPE_BASE = 10000.0
NORM_EPS = 1e-6
CORES = 2
WINDOW_ALIGN = 16
MESH = pl.DeviceIdType.MESH
F32 = jnp.float32
BF16 = jnp.bfloat16
ANY = pl.BlockSpec(memory_space=pl.ANY)
VMEM = pl.BlockSpec(memory_space=pltpu.VMEM)
SMEM = pl.BlockSpec(memory_space=pltpu.SMEM)


def dot(a, b):
    return lax.dot_general(a, b, (((1,), (0,)), ((), ())), preferred_element_type=F32)


def dot_t(a, b):
    return lax.dot_general(a, b, (((1,), (1,)), ((), ())), preferred_element_type=F32)


def exchange_kernel(
    chips, steps, plen_ref, k_ref, v_ref, x_ref, gain_ref, wq_ref, wk_ref, wv_ref, wo_ref, cos_ref, sin_ref,
    kf, vf, kn, vn, yf,
    stage, xs, gs, cs, sn, hs, wb, wo_own, wo_peer, qs, sc, pb, pn, o_own, o_peer, yp, rs,
    kv_send, kv_recv, kv_own, w_sem, in_sem, wo_sems, o_send, o_recv, rs_send, rs_recv, ag_send, ag_recv, d_send, d_recv,
):
    rows, heads, _, head_dim = kn.shape
    out_len = kf.shape[2]
    shard = k_ref.shape[2]
    seq_len = out_len - steps
    parts = chips * CORES
    model = wq_ref.shape[0]
    width = heads * head_dim
    half = model // CORES
    block = half // chips
    group = lax.axis_index("dp")
    me = lax.axis_index("tp")
    chip, core = me // CORES, lax.rem(me, CORES)
    partner = chip * CORES + (1 - core)

    hops = [(1, 0), (chips - 1, 0)] + [(d, 0) for d in range(2, chips - 1)]
    hops += [(1, 1), (chips - 1, 1)] + [(d, 1) for d in range(2, chips - 1)] + [(0, 1)]

    def peer(hop):
        return lax.rem(chip + hop[0], chips) * CORES + lax.rem(core + hop[1], CORES)

    def remote(src, dst, send, recv, target):
        return pltpu.make_async_remote_copy(src_ref=src, dst_ref=dst, send_sem=send, recv_sem=recv, device_id=(group, target), device_id_type=MESH)

    barrier = pltpu.get_barrier_semaphore()
    for hop in hops:
        pl.semaphore_signal(barrier, inc=1, device_id=(group, peer(hop)), device_id_type=MESH)
    pl.semaphore_wait(barrier, parts - 1)

    slots = pl.ds(pl.multiple_of(me * shard, shard), shard)

    def cache_copy(kind, b, n):
        src, dst = ((k_ref, kf), (v_ref, vf))[kind]
        target = peer(hops[n])
        return remote(src.at[b, pl.ds(target * heads, heads)], dst.at[b, :, slots, :], kv_send.at[kind, b, n], kv_recv.at[kind, b, n], target)

    def own_copy(kind, b):
        src, dst = ((k_ref, kf), (v_ref, vf))[kind]
        return pltpu.make_async_copy(src.at[b, pl.ds(me * heads, heads)], dst.at[b, :, slots, :], kv_own.at[kind, b])

    def half_cols(which):
        return pl.ds(pl.multiple_of(which * half, half), half)

    wo_send = remote(wo_ref.at[:, half_cols(1 - core)], wo_peer, wo_sems.at[0], wo_sems.at[1], partner)
    wo_send.start()
    for b in range(rows):
        for kind in range(2):
            for n in range(len(hops)):
                cache_copy(kind, b, n).start()

    loads = [
        pltpu.make_async_copy(gain_ref, gs, in_sem.at[0]),
        pltpu.make_async_copy(cos_ref, cs, in_sem.at[1]),
        pltpu.make_async_copy(sin_ref, sn, in_sem.at[2]),
        pltpu.make_async_copy(wo_ref.at[:, half_cols(core)], wo_own, in_sem.at[3]),
    ]
    for c in loads:
        c.start()
    pair = wb.shape[2]
    groups = width // pair
    w_loads = [
        pltpu.make_async_copy((wq_ref, wk_ref, wv_ref)[i // groups].at[:, i % groups * pair:(i % groups + 1) * pair], wb.at[i % 2], w_sem.at[i])
        for i in range(3 * groups)
    ]
    w_loads[0].start()
    w_loads[1].start()
    for b in range(rows):
        for kind in range(2):
            own_copy(kind, b).start()
    zero_tail = jnp.zeros((rows, heads, steps, head_dim), BF16)
    kf[:, :, seq_len:, :] = zero_tail
    vf[:, :, seq_len:, :] = zero_tail
    for c in loads:
        c.wait()

    gain = 1.0 + gs[...].astype(F32)
    part_steps = stage.shape[0]
    for t in range(0, steps, part_steps):
        x_load = pltpu.make_async_copy(x_ref.at[t:t + part_steps], stage, in_sem.at[4])
        x_load.start()
        x_load.wait()
        for b in range(rows):
            x = stage[:, b, :]
            xs[b, t:t + part_steps, :] = x
            residual = x.astype(F32)
            inv_rms = lax.rsqrt(jnp.mean(residual * residual, axis=-1, keepdims=True) + NORM_EPS)
            hs[b * steps + t:b * steps + t + part_steps, :] = (residual * inv_rms * gain).astype(BF16)

    for i, load in enumerate(w_loads):
        load.wait()
        matrix, j = i // groups, i % groups
        flat = dot(hs[...], wb[i % 2]).astype(BF16)
        if i + 2 < len(w_loads):
            w_loads[i + 2].start()
        for sub in range(pair // head_dim):
            for b in range(rows):
                u = flat[b * steps:(b + 1) * steps, sub * head_dim:(sub + 1) * head_dim]
                if matrix < 2:
                    u = u.astype(F32)
                    u = u * cs[b] + pltpu.roll(u, head_dim // 2, 1) * sn[b]
                    if matrix == 0:
                        u = u * head_dim ** -0.5
                (qs, kn, vn)[matrix][b, j * (pair // head_dim) + sub] = u.astype(BF16)

    wo_send.wait()
    causal = lax.broadcasted_iota(jnp.int32, (steps, steps), 1) <= lax.broadcasted_iota(jnp.int32, (steps, steps), 0)
    slot_id = lax.broadcasted_iota(jnp.int32, (steps, shard), 1)

    def rs_copy(b, d):
        to = lax.rem(chip + d, chips)
        return remote(yp.at[b, :, pl.ds(pl.multiple_of(to * block, block), block)], rs.at[b, d - 1], rs_send.at[b, d - 1], rs_recv.at[b, d - 1], to * CORES + core)

    def o_copy(b):
        return remote(o_own.at[b], o_peer.at[b], o_send.at[b], o_recv.at[b], partner)

    @pl.loop(0, rows)
    def _(b):
        own_copy(0, b).wait()
        for n in range(len(hops)):
            cache_copy(0, b, n).wait_recv()
        length = plen_ref[b]

        @pl.loop(0, heads)
        def _(h):
            q = qs[b, h]
            peak = jnp.full((steps, shard), -jnp.inf, F32)
            for s in range(parts):
                scores = dot_t(q, kf[b, h, s * shard:(s + 1) * shard, :])
                scores = jnp.where(slot_id < length - s * shard, scores, -jnp.inf)
                sc[:, s * shard:(s + 1) * shard] = scores
                peak = jnp.maximum(peak, scores)
            fresh = jnp.where(causal, dot_t(q, kn[b, h]), -jnp.inf)
            row_peak = jnp.maximum(jnp.max(peak, axis=-1, keepdims=True), jnp.max(fresh, axis=-1, keepdims=True))
            total = jnp.zeros((steps, shard), F32)
            for s in range(parts):
                e = jnp.exp(sc[:, s * shard:(s + 1) * shard] - row_peak)
                sc[:, s * shard:(s + 1) * shard] = e
                total = total + e
            fresh = jnp.exp(fresh - row_peak)
            inv = 1.0 / (jnp.sum(total, axis=-1, keepdims=True) + jnp.sum(fresh, axis=-1, keepdims=True))
            for s in range(parts):
                pb[h, :, s * shard:(s + 1) * shard] = (sc[:, s * shard:(s + 1) * shard] * inv).astype(BF16)
            pn[h] = (fresh * inv).astype(BF16)

        own_copy(1, b).wait()
        for n in range(len(hops)):
            cache_copy(1, b, n).wait_recv()

        for h in range(heads):
            out = dot(pn[h], vn[b, h]) + dot(pb[h], vf[b, h, :seq_len, :])
            o_own[b, :, h * head_dim:(h + 1) * head_dim] = out.astype(BF16)
        o_copy(b).start()
        o_copy(b).wait_recv()
        for j in range(chips):
            cols = slice(j * block, (j + 1) * block)
            part = dot(o_own[b], wo_own[:, cols]) + dot(o_peer[b], wo_peer[:, cols])
            yp[b, :, cols] = part.astype(BF16)
        for d in range(1, chips):
            rs_copy(b, d).start()

    def columns(which_core, which_chip):
        return pl.ds(pl.multiple_of(which_core * half + which_chip * block, block), block)

    def ag_copy(b, d):
        to = lax.rem(chip + d, chips)
        mine = yf.at[b, :, columns(core, chip)]
        return remote(mine, mine, ag_send.at[b, d - 1], ag_recv.at[b, d - 1], to * CORES + core)

    def d_copy(b):
        mine = yf.at[b, :, half_cols(core)]
        return remote(mine, mine, d_send.at[b], d_recv.at[b], partner)

    for b in range(rows):
        for d in range(1, chips):
            rs_copy(b, d).wait_recv()
        attn = yp[b, :, pl.ds(pl.multiple_of(chip * block, block), block)].astype(F32)
        for d in range(1, chips):
            attn = attn + rs[b, d - 1].astype(F32)
        yf[b, :, columns(core, chip)] = (xs[b, :, columns(core, chip)].astype(F32) + attn).astype(BF16)
        for d in range(1, chips):
            ag_copy(b, d).start()
    for b in range(rows):
        for d in range(1, chips):
            ag_copy(b, d).wait_recv()
        d_copy(b).start()
    for b in range(rows):
        d_copy(b).wait()
        o_copy(b).wait_send()
        for d in range(1, chips):
            rs_copy(b, d).wait_send()
            ag_copy(b, d).wait_send()
        for kind in range(2):
            for n in range(len(hops)):
                cache_copy(kind, b, n).wait_send()


def write_kernel(plen_ref, kf, vf, kn, vn, yf, k_out, v_out, y_out, win, ys, big_sem, win_sem, y_sem):
    rows, heads, steps, head_dim = kn.shape
    out_len = kf.shape[2]
    span = win.shape[3]
    last = out_len - span

    def start_of(b):
        p = plen_ref[b]
        return pl.multiple_of(jnp.minimum(p - lax.rem(p, WINDOW_ALIGN), last), WINDOW_ALIGN)

    def big(kind, b):
        src, dst = ((kf, k_out), (vf, v_out))[kind]
        return pltpu.make_async_copy(src.at[b], dst.at[b], big_sem.at[kind, b])

    def small(kind, b):
        return pltpu.make_async_copy(win.at[kind, b], (k_out, v_out)[kind].at[b, :, pl.ds(start_of(b), span), :], win_sem.at[kind, b])

    for b in range(rows):
        for kind in range(2):
            big(kind, b).start()
    for b in range(rows):
        ys[:, b, :] = yf[b]
    y_copy = pltpu.make_async_copy(ys, y_out, y_sem)
    y_copy.start()
    row_id = lax.broadcasted_iota(jnp.int32, (span, steps), 0)
    col_id = lax.broadcasted_iota(jnp.int32, (span, steps), 1)
    pos = lax.broadcasted_iota(jnp.int32, (span, head_dim), 0)
    for b in range(rows):
        start = start_of(b)
        offset = plen_ref[b] - start
        select = (row_id == col_id + offset).astype(BF16)
        fresh = (pos >= offset) & (pos < offset + steps)
        for kind in range(2):
            old, new = ((kf, kn), (vf, vn))[kind]
            for h in range(heads):
                moved = dot(select, new[b, h])
                kept = old[b, h, pl.ds(start, span), :].astype(F32)
                win[kind, b, h] = jnp.where(fresh, moved, kept).astype(BF16)
    for b in range(rows):
        for kind in range(2):
            big(kind, b).wait()
            small(kind, b).start()
    y_copy.wait()
    for b in range(rows):
        for kind in range(2):
            small(kind, b).wait()


def solution(mesh):
    parts = mesh.shape["tp"]
    chips = parts // CORES

    def local_block(k_cache, v_cache, prompt_len, x_steps, w_norm, w_q, w_k, w_v, w_o):
        rows, _, shard, head_dim = k_cache.shape
        steps, _, model = x_steps.shape
        width = w_q.shape[1]
        heads = width // head_dim
        seq_len = shard * parts
        out_len = seq_len + steps
        half = model // CORES
        block = half // chips
        half_dim = head_dim // 2
        inv_freq = ROPE_BASE ** (-2.0 * jnp.arange(half_dim, dtype=F32) / head_dim)
        positions = prompt_len[:, None] + jnp.arange(steps)[None, :]
        angles = positions.astype(F32)[..., None] * inv_freq
        cos, sin = jnp.cos(angles), jnp.sin(angles)
        cos_full = jnp.concatenate([cos, cos], axis=-1)
        sin_full = jnp.concatenate([-sin, sin], axis=-1)
        dma = pltpu.SemaphoreType.DMA
        peers = parts - 1
        kf, vf, kn, vn, yf = pl.pallas_call(
            functools.partial(exchange_kernel, chips, steps),
            out_shape=(
                pltpu.VMEM((rows, heads, out_len, head_dim), BF16),
                pltpu.VMEM((rows, heads, out_len, head_dim), BF16),
                pltpu.VMEM((rows, heads, steps, head_dim), BF16),
                pltpu.VMEM((rows, heads, steps, head_dim), BF16),
                pltpu.VMEM((rows, steps, model), BF16),
            ),
            in_specs=[SMEM] + [ANY] * 10,
            out_specs=(VMEM,) * 5,
            scratch_shapes=[
                pltpu.VMEM((WINDOW_ALIGN, rows, model), BF16),
                pltpu.VMEM((rows, steps, model), BF16),
                pltpu.VMEM((1, model), BF16),
                pltpu.VMEM((rows, steps, head_dim), F32),
                pltpu.VMEM((rows, steps, head_dim), F32),
                pltpu.VMEM((rows * steps, model), BF16),
                pltpu.VMEM((2, model, 2 * head_dim), BF16),
                pltpu.VMEM((width, half), BF16),
                pltpu.VMEM((width, half), BF16),
                pltpu.VMEM((rows, heads, steps, head_dim), BF16),
                pltpu.VMEM((steps, seq_len), F32),
                pltpu.VMEM((heads, steps, seq_len), BF16),
                pltpu.VMEM((heads, steps, steps), BF16),
                pltpu.VMEM((rows, steps, width), BF16),
                pltpu.VMEM((rows, steps, width), BF16),
                pltpu.VMEM((rows, steps, half), BF16),
                pltpu.VMEM((rows, chips - 1, steps, block), BF16),
                dma((2, rows, peers)),
                dma((2, rows, peers)),
                dma((2, rows)),
                dma((6,)),
                dma((5,)),
                dma((2,)),
                dma((rows,)),
                dma((rows,)),
                dma((rows, chips - 1)),
                dma((rows, chips - 1)),
                dma((rows, chips - 1)),
                dma((rows, chips - 1)),
                dma((rows,)),
                dma((rows,)),
            ],
            compiler_params=pltpu.CompilerParams(collective_id=0, has_side_effects=True, vmem_limit_bytes=28 << 20),
        )(prompt_len, k_cache, v_cache, x_steps, w_norm.reshape(1, model), w_q, w_k, w_v, w_o, cos_full, sin_full)
        span = steps + WINDOW_ALIGN
        k_out, v_out, y = pl.pallas_call(
            write_kernel,
            out_shape=(
                jax.ShapeDtypeStruct((rows, heads, out_len, head_dim), BF16),
                jax.ShapeDtypeStruct((rows, heads, out_len, head_dim), BF16),
                jax.ShapeDtypeStruct((steps, rows, model), BF16),
            ),
            in_specs=[SMEM] + [VMEM] * 5,
            out_specs=(ANY,) * 3,
            scratch_shapes=[
                pltpu.VMEM((2, rows, heads, span, head_dim), BF16),
                pltpu.VMEM((steps, rows, model), BF16),
                dma((2, rows)),
                dma((2, rows)),
                dma,
            ],
            compiler_params=pltpu.CompilerParams(vmem_limit_bytes=16 << 20),
        )(prompt_len, kf, vf, kn, vn, yf)
        return y, k_out, v_out

    cache_spec = P("dp", None, "tp", None)
    col_spec = P(None, "tp")
    out_cache_spec = P("dp", "tp", None, None)
    return jax.shard_map(local_block, mesh=mesh, in_specs=(cache_spec, cache_spec, P("dp"), P(None, "dp", None), P(None), col_spec, col_spec, col_spec, P("tp", None)), out_specs=(P(None, "dp", None), out_cache_spec, out_cache_spec), check_vma=False)
```

```python
import functools

import jax
import jax.numpy as jnp
import numpy as np
from jax import lax
from jax.experimental import pallas as pl
from jax.experimental.pallas import tpu as pltpu
from jax.sharding import PartitionSpec as P

ROPE_BASE = 10000.0
NORM_EPS = 1e-6
CORES = 2
WINDOW_ALIGN = 16
STAGE_STEPS = 8
VMEM_LIMIT = 12480 << 10
MESH = pl.DeviceIdType.MESH
F32 = jnp.float32
BF16 = jnp.bfloat16
ANY = pl.BlockSpec(memory_space=pl.ANY)
VMEM = pl.BlockSpec(memory_space=pltpu.VMEM)
SMEM = pl.BlockSpec(memory_space=pltpu.SMEM)


def dot(a, b):
    return lax.dot_general(a, b, (((1,), (0,)), ((), ())), preferred_element_type=F32)


def dot_t(a, b):
    return lax.dot_general(a, b, (((1,), (1,)), ((), ())), preferred_element_type=F32)


def exchange_kernel(
    chips, steps, plen_ref, k_ref, v_ref, x_ref, gain_ref, wq_ref, wk_ref, wv_ref, wo_ref, cos_ref, sin_ref,
    kf, vf, kn, vn, yf,
    stage, gs, hp, wb, sc, pn, xs, wo_own, wo_peer, qs, o_peer, rs,
    kv_send, kv_recv, kv_own, w_sem, in_sem, wo_sems, o_send, o_recv, rs_send, rs_recv, ag_send, ag_recv, d_send, d_recv,
):
    rows, heads, _, head_dim = kn.shape
    out_len = kf.shape[2]
    shard = k_ref.shape[2]
    seq_len = out_len - steps
    parts = chips * CORES
    model = wq_ref.shape[0]
    width = heads * head_dim
    half = model // CORES
    block = half // chips
    group = lax.axis_index("dp")
    me = lax.axis_index("tp")
    chip, core = me // CORES, lax.rem(me, CORES)
    partner = chip * CORES + (1 - core)

    hops = [(1, 0), (chips - 1, 0)] + [(d, 0) for d in range(2, chips - 1)]
    hops += [(1, 1), (chips - 1, 1)] + [(d, 1) for d in range(2, chips - 1)] + [(0, 1)]

    def peer(hop):
        return lax.rem(chip + hop[0], chips) * CORES + lax.rem(core + hop[1], CORES)

    def remote(src, dst, send, recv, target):
        return pltpu.make_async_remote_copy(src_ref=src, dst_ref=dst, send_sem=send, recv_sem=recv, device_id=(group, target), device_id_type=MESH)

    barrier = pltpu.get_barrier_semaphore()
    for hop in hops:
        pl.semaphore_signal(barrier, inc=1, device_id=(group, peer(hop)), device_id_type=MESH)
    pl.semaphore_wait(barrier, parts - 1)

    slots = pl.ds(pl.multiple_of(me * shard, shard), shard)

    def cache_copy(kind, b, n):
        src, dst = ((k_ref, kf), (v_ref, vf))[kind]
        target = peer(hops[n])
        return remote(src.at[b, pl.ds(target * heads, heads)], dst.at[b, :, slots, :], kv_send.at[kind, b, n], kv_recv.at[kind, b, n], target)

    def own_copy(kind, b):
        src, dst = ((k_ref, kf), (v_ref, vf))[kind]
        return pltpu.make_async_copy(src.at[b, pl.ds(me * heads, heads)], dst.at[b, :, slots, :], kv_own.at[kind, b])

    def half_cols(which):
        return pl.ds(pl.multiple_of(which * half, half), half)

    wo_send = remote(wo_ref.at[:, half_cols(1 - core)], wo_peer, wo_sems.at[0], wo_sems.at[1], partner)
    wo_send.start()
    for b in range(rows):
        for kind in range(2):
            for n in range(len(hops)):
                cache_copy(kind, b, n).start()

    for b in range(rows):
        for kind in range(2):
            own_copy(kind, b).start()
    wo_load = pltpu.make_async_copy(wo_ref.at[:, half_cols(core)], wo_own, in_sem.at[3])
    wo_load.start()
    zero_tail = jnp.zeros((rows, heads, steps, head_dim), BF16)
    kf[:, :, seq_len:, :] = zero_tail
    vf[:, :, seq_len:, :] = zero_tail

    def columns(which_core, which_chip):
        return pl.ds(pl.multiple_of(which_core * half + which_chip * block, block), block)

    loads = [
        pltpu.make_async_copy(gain_ref, gs, in_sem.at[0]),
        pltpu.make_async_copy(cos_ref, sc.at[:, :rows * head_dim], in_sem.at[1]),
        pltpu.make_async_copy(sin_ref, sc.at[:, rows * head_dim:2 * rows * head_dim], in_sem.at[2]),
    ]
    for c in loads:
        c.start()
    groups = width // head_dim
    w_loads = [
        pltpu.make_async_copy((wq_ref, wk_ref, wv_ref)[i // groups].at[:, i % groups * head_dim:(i % groups + 1) * head_dim], wb.at[i % 2], w_sem.at[i])
        for i in range(3 * groups)
    ]
    w_loads[0].start()
    w_loads[1].start()
    for c in loads:
        c.wait()

    part_steps = stage.shape[0]
    for t in range(0, steps, part_steps):
        x_load = pltpu.make_async_copy(x_ref.at[t:t + part_steps], stage, in_sem.at[4])
        x_load.start()
        x_load.wait()

        for b in range(rows):
            xs[b, t:t + part_steps, :] = stage[:, b, columns(core, chip)]
            squares = jnp.zeros((part_steps, block), F32)
            for c in range(0, model, block):
                residual = stage[:, b, c:c + block].astype(F32)
                squares = squares + residual * residual
            inv_rms = lax.rsqrt(jnp.sum(squares, axis=-1, keepdims=True) * (1.0 / model) + NORM_EPS)
            for c in range(0, model, block):
                residual = stage[:, b, c:c + block].astype(F32)
                gain = 1.0 + gs[c:c + block].astype(F32).reshape(1, block)
                hp[b * steps + t:b * steps + t + part_steps, c:c + block] = (residual * inv_rms * gain).astype(BF16)

    def lane_tile(n):
        return pl.ds(pl.multiple_of(n * head_dim, head_dim), head_dim)

    for i, load in enumerate(w_loads):
        load.wait()
        matrix, j = i // groups, i % groups

        @pl.loop(0, rows)
        def _(b, i=i, matrix=matrix, j=j):
            u = dot(hp[pl.ds(pl.multiple_of(b * steps, steps), steps), :model], wb[i % 2]).astype(BF16)
            if matrix < 2:
                u = u.astype(F32)
                u = u * sc[:, lane_tile(b)] + pltpu.roll(u, head_dim // 2, 1) * sc[:, lane_tile(rows + b)]
                if matrix == 0:
                    u = u * head_dim ** -0.5
            (qs, kn, vn)[matrix][b, j] = u.astype(BF16)

        if i + 2 < len(w_loads):
            w_loads[i + 2].start()

    wo_load.wait()
    wo_send.wait()
    causal = lax.broadcasted_iota(jnp.int32, (steps, steps), 1) <= lax.broadcasted_iota(jnp.int32, (steps, steps), 0)
    slot_id = lax.broadcasted_iota(jnp.int32, (steps, shard), 1)

    lanes = wb.shape[2]
    tiles = block // lanes

    def head_rows(h):
        return pl.ds(pl.multiple_of(h * steps, steps), steps)

    def partial_rows(b, which_chip, tile=0, count=1):
        first = ((b * chips + which_chip) * tiles + tile) * steps
        return pl.ds(pl.multiple_of(first, steps), count * steps)

    def rs_copy(b, d):
        to = lax.rem(chip + d, chips)
        return remote(wb.at[0, partial_rows(b, to, 0, tiles)], rs.at[b, d - 1], rs_send.at[b, d - 1], rs_recv.at[b, d - 1], to * CORES + core)

    def head_tile(b, h, count=1):
        return pl.ds(pl.multiple_of((b * heads + h) * steps, steps), count * steps)

    def o_copy(b):
        return remote(wb.at[1, head_tile(b, 0, heads)], o_peer.at[b], o_send.at[b], o_recv.at[b], partner)

    @pl.loop(0, rows)
    def _(b):
        own_copy(0, b).wait()
        for n in range(len(hops)):
            cache_copy(0, b, n).wait_recv()
        length = plen_ref[b]

        @pl.loop(0, heads)
        def _(h):
            q = qs[b, h]

            def score(s, peak):
                cols = pl.ds(pl.multiple_of(s * shard, shard), shard)
                scores = dot_t(q, kf[b, h, cols, :])
                scores = jnp.where(slot_id < length - s * shard, scores, -jnp.inf)
                sc[:, cols] = scores
                return jnp.maximum(peak, scores)

            peak = lax.fori_loop(0, parts, score, jnp.full((steps, shard), -jnp.inf, F32))
            fresh = jnp.where(causal, dot_t(q, kn[b, h]), -jnp.inf)
            row_peak = jnp.maximum(jnp.max(peak, axis=-1, keepdims=True), jnp.max(fresh, axis=-1, keepdims=True))

            def exponent(s, total):
                cols = pl.ds(pl.multiple_of(s * shard, shard), shard)
                e = jnp.exp(sc[:, cols] - row_peak)
                sc[:, cols] = e
                return total + e

            total = lax.fori_loop(0, parts, exponent, jnp.zeros((steps, shard), F32))
            fresh = jnp.exp(fresh - row_peak)
            inv = 1.0 / (jnp.sum(total, axis=-1, keepdims=True) + jnp.sum(fresh, axis=-1, keepdims=True))

            @pl.loop(0, parts)
            def _(s):
                cols = pl.ds(pl.multiple_of(s * shard, shard), shard)
                hp[head_rows(h), cols] = (sc[:, cols] * inv).astype(BF16)

            pn[h] = (fresh * inv).astype(BF16)

        own_copy(1, b).wait()
        for n in range(len(hops)):
            cache_copy(1, b, n).wait_recv()

        @pl.loop(0, heads)
        def _(h):
            out = dot(pn[h], vn[b, h])
            for s in range(parts):
                cols = slice(s * shard, (s + 1) * shard)
                out = out + dot(hp[head_rows(h), cols], vf[b, h, cols, :])
            wb[1, head_tile(b, h)] = out.astype(BF16)

        o_copy(b).start()
        o_copy(b).wait_recv()

        @pl.loop(0, chips)
        def _(j):
            cols = pl.ds(pl.multiple_of(j * block, block), block)
            own = jnp.concatenate([wb[1, head_tile(b, h)] for h in range(heads)], axis=1)
            other = jnp.concatenate([o_peer[b, h * steps:(h + 1) * steps] for h in range(heads)], axis=1)
            part = (dot(own, wo_own[:, cols]) + dot(other, wo_peer[:, cols])).astype(BF16)
            for tile in range(tiles):
                wb[0, partial_rows(b, j, tile)] = part[:, tile * lanes:(tile + 1) * lanes]

        for d in range(1, chips):
            rs_copy(b, d).start()

    def ag_copy(b, d):
        to = lax.rem(chip + d, chips)
        mine = yf.at[b, :, columns(core, chip)]
        return remote(mine, mine, ag_send.at[b, d - 1], ag_recv.at[b, d - 1], to * CORES + core)

    def d_copy(b):
        mine = yf.at[b, :, half_cols(core)]
        return remote(mine, mine, d_send.at[b], d_recv.at[b], partner)

    for b in range(rows):
        for d in range(1, chips):
            rs_copy(b, d).wait_recv()
        for tile in range(tiles):
            cols = slice(tile * lanes, (tile + 1) * lanes)
            attn = wb[0, partial_rows(b, chip, tile)].astype(F32)
            for d in range(1, chips):
                attn = attn + rs[b, d - 1, tile * steps:(tile + 1) * steps].astype(F32)
            out_cols = pl.ds(pl.multiple_of(core * half + chip * block + tile * lanes, lanes), lanes)
            yf[b, :, out_cols] = (xs[b, :, cols].astype(F32) + attn).astype(BF16)
        for d in range(1, chips):
            ag_copy(b, d).start()
    for b in range(rows):
        for d in range(1, chips):
            ag_copy(b, d).wait_recv()
        d_copy(b).start()
    for b in range(rows):
        d_copy(b).wait()
        o_copy(b).wait_send()
        for d in range(1, chips):
            rs_copy(b, d).wait_send()
            ag_copy(b, d).wait_send()
        for kind in range(2):
            for n in range(len(hops)):
                cache_copy(kind, b, n).wait_send()


def write_kernel(plen_ref, kf, vf, kn, vn, yf, k_out, v_out, y_out, win, ys, big_sem, win_sem, y_sem):
    rows, heads, steps, head_dim = kn.shape
    out_len = kf.shape[2]
    span = win.shape[3]
    last = out_len - span

    def start_of(b):
        p = plen_ref[b]
        return pl.multiple_of(jnp.minimum(p - lax.rem(p, WINDOW_ALIGN), last), WINDOW_ALIGN)

    def big(kind, b):
        src, dst = ((kf, k_out), (vf, v_out))[kind]
        return pltpu.make_async_copy(src.at[b], dst.at[b], big_sem.at[kind, b])

    def small(kind, b):
        return pltpu.make_async_copy(win.at[kind, b], (k_out, v_out)[kind].at[b, :, pl.ds(start_of(b), span), :], win_sem.at[kind, b])

    for b in range(rows):
        for kind in range(2):
            big(kind, b).start()
    for b in range(rows):
        ys[:, b, :] = yf[b]
    y_copy = pltpu.make_async_copy(ys, y_out, y_sem)
    y_copy.start()
    row_id = lax.broadcasted_iota(jnp.int32, (span, steps), 0)
    col_id = lax.broadcasted_iota(jnp.int32, (span, steps), 1)
    pos = lax.broadcasted_iota(jnp.int32, (span, head_dim), 0)
    for b in range(rows):
        start = start_of(b)
        offset = plen_ref[b] - start
        select = (row_id == col_id + offset).astype(BF16)
        fresh = (pos >= offset) & (pos < offset + steps)
        for kind in range(2):
            old, new = ((kf, kn), (vf, vn))[kind]
            for h in range(heads):
                moved = dot(select, new[b, h])
                kept = old[b, h, pl.ds(start, span), :].astype(F32)
                win[kind, b, h] = jnp.where(fresh, moved, kept).astype(BF16)
    for b in range(rows):
        for kind in range(2):
            big(kind, b).wait()
            small(kind, b).start()
    y_copy.wait()
    for b in range(rows):
        for kind in range(2):
            small(kind, b).wait()


def solution(mesh):
    parts = mesh.shape["tp"]
    chips = parts // CORES

    def local_block(k_cache, v_cache, prompt_len, x_steps, w_norm, w_q, w_k, w_v, w_o):
        rows, _, shard, head_dim = k_cache.shape
        steps, _, model = x_steps.shape
        width = w_q.shape[1]
        heads = width // head_dim
        seq_len = shard * parts
        out_len = seq_len + steps
        half = model // CORES
        block = half // chips
        tiles = block // head_dim
        half_dim = head_dim // 2
        inv_freq = (ROPE_BASE ** (-2.0 * np.arange(half_dim) / head_dim)).astype(np.float32)
        sign = np.where(np.arange(head_dim) < half_dim, -1.0, 1.0).astype(np.float32)
        starts = jnp.broadcast_to(prompt_len[:, None], (rows, head_dim)).reshape(1, rows * head_dim)
        angles = (jnp.arange(steps)[:, None] + starts).astype(F32) * np.tile(inv_freq, 2 * rows)
        cos, sin = jnp.cos(angles), jnp.sin(angles) * np.tile(sign, rows)
        dma = pltpu.SemaphoreType.DMA
        peers = parts - 1
        kf, vf, kn, vn, yf = pl.pallas_call(
            functools.partial(exchange_kernel, chips, steps),
            out_shape=(
                pltpu.VMEM((rows, heads, out_len, head_dim), BF16),
                pltpu.VMEM((rows, heads, out_len, head_dim), BF16),
                pltpu.VMEM((rows, heads, steps, head_dim), BF16),
                pltpu.VMEM((rows, heads, steps, head_dim), BF16),
                pltpu.VMEM((rows, steps, model), BF16),
            ),
            in_specs=[SMEM] + [ANY] * 10,
            out_specs=(VMEM,) * 5,
            scratch_shapes=[
                pltpu.VMEM((STAGE_STEPS, rows, model), BF16),
                pltpu.VMEM((model,), BF16),
                pltpu.VMEM((max(rows, heads) * steps, max(model, seq_len)), BF16),
                pltpu.VMEM((2, model, head_dim), BF16),
                pltpu.VMEM((steps, seq_len), F32),
                pltpu.VMEM((heads, steps, steps), BF16),
                pltpu.VMEM((rows, steps, block), BF16),
                pltpu.VMEM((width, half), BF16),
                pltpu.VMEM((width, half), BF16),
                pltpu.VMEM((rows, heads, steps, head_dim), BF16),
                pltpu.VMEM((rows, heads * steps, head_dim), BF16),
                pltpu.VMEM((rows, chips - 1, tiles * steps, head_dim), BF16),
                dma((2, rows, peers)),
                dma((2, rows, peers)),
                dma((2, rows)),
                dma((3 * width // head_dim,)),
                dma((5,)),
                dma((2,)),
                dma((rows,)),
                dma((rows,)),
                dma((rows, chips - 1)),
                dma((rows, chips - 1)),
                dma((rows, chips - 1)),
                dma((rows, chips - 1)),
                dma((rows,)),
                dma((rows,)),
            ],
            compiler_params=pltpu.CompilerParams(collective_id=0, has_side_effects=True, vmem_limit_bytes=VMEM_LIMIT),
        )(prompt_len, *(pltpu.with_memory_space_constraint(a, pltpu.HBM) for a in (k_cache, v_cache, x_steps, w_norm, w_q, w_k, w_v, w_o)), cos, sin)
        span = steps + WINDOW_ALIGN
        k_out, v_out, y = pl.pallas_call(
            write_kernel,
            out_shape=(
                jax.ShapeDtypeStruct((rows, heads, out_len, head_dim), BF16),
                jax.ShapeDtypeStruct((rows, heads, out_len, head_dim), BF16),
                jax.ShapeDtypeStruct((steps, rows, model), BF16),
            ),
            in_specs=[SMEM] + [VMEM] * 5,
            out_specs=(ANY,) * 3,
            scratch_shapes=[
                pltpu.VMEM((2, rows, heads, span, head_dim), BF16),
                pltpu.VMEM((steps, rows, model), BF16),
                dma((2, rows)),
                dma((2, rows)),
                dma,
            ],
            compiler_params=pltpu.CompilerParams(vmem_limit_bytes=6 << 20),
        )(prompt_len, kf, vf, kn, vn, yf)
        return y, k_out, v_out

    cache_spec = P("dp", None, "tp", None)
    col_spec = P(None, "tp")
    out_cache_spec = P("dp", "tp", None, None)
    return jax.shard_map(local_block, mesh=mesh, in_specs=(cache_spec, cache_spec, P("dp"), P(None, "dp", None), P(None), col_spec, col_spec, col_spec, P("tp", None)), out_specs=(P(None, "dp", None), out_cache_spec, out_cache_spec), check_vma=False)
```

```python
import functools

import jax
import jax.numpy as jnp
import numpy as np
from jax import lax
from jax.experimental import pallas as pl
from jax.experimental.pallas import tpu as pltpu
from jax.sharding import PartitionSpec as P

ROPE_BASE = 10000.0
NORM_EPS = 1e-6
CORES = 2
WINDOW_ALIGN = 16
STAGE_STEPS = 8
VMEM_LIMIT = 12480 << 10
MESH = pl.DeviceIdType.MESH
F32 = jnp.float32
BF16 = jnp.bfloat16
ANY = pl.BlockSpec(memory_space=pl.ANY)
VMEM = pl.BlockSpec(memory_space=pltpu.VMEM)


def dot(a, b):
    return lax.dot_general(a, b, (((1,), (0,)), ((), ())), preferred_element_type=F32)


def dot_t(a, b):
    return lax.dot_general(a, b, (((1,), (1,)), ((), ())), preferred_element_type=F32)


def exchange_kernel(
    chips, steps, plen_hbm, k_ref, v_ref, x_ref, gain_ref, wq_ref, wk_ref, wv_ref, wo_ref, freq_ref,
    kf, vf, kn, vn, yf,
    plen_ref, freq, stage, gs, hp, wb, sc, pn, xs, wo_own, wo_peer, qs, o_peer, rs,
    kv_send, kv_recv, kv_own, w_sem, in_sem, wo_sems, o_send, o_recv, rs_send, rs_recv, ag_send, ag_recv, d_send, d_recv,
):
    rows, heads, _, head_dim = kn.shape
    out_len = kf.shape[2]
    shard = k_ref.shape[2]
    seq_len = out_len - steps
    parts = chips * CORES
    model = wq_ref.shape[0]
    width = heads * head_dim
    half = model // CORES
    block = half // chips
    group = lax.axis_index("dp")
    me = lax.axis_index("tp")
    chip, core = me // CORES, lax.rem(me, CORES)
    partner = chip * CORES + (1 - core)

    hops = [(1, 0), (chips - 1, 0)] + [(d, 0) for d in range(2, chips - 1)]
    hops += [(1, 1), (chips - 1, 1)] + [(d, 1) for d in range(2, chips - 1)] + [(0, 1)]

    def peer(hop):
        return lax.rem(chip + hop[0], chips) * CORES + lax.rem(core + hop[1], CORES)

    def remote(src, dst, send, recv, target):
        return pltpu.make_async_remote_copy(src_ref=src, dst_ref=dst, send_sem=send, recv_sem=recv, device_id=(group, target), device_id_type=MESH)

    barrier = pltpu.get_barrier_semaphore()
    for hop in hops:
        pl.semaphore_signal(barrier, inc=1, device_id=(group, peer(hop)), device_id_type=MESH)
    pl.semaphore_wait(barrier, parts - 1)

    slots = pl.ds(pl.multiple_of(me * shard, shard), shard)

    def cache_copy(kind, b, n):
        src, dst = ((k_ref, kf), (v_ref, vf))[kind]
        target = peer(hops[n])
        return remote(src.at[b, pl.ds(target * heads, heads)], dst.at[b, :, slots, :], kv_send.at[kind, b, n], kv_recv.at[kind, b, n], target)

    def own_copy(kind, b):
        src, dst = ((k_ref, kf), (v_ref, vf))[kind]
        return pltpu.make_async_copy(src.at[b, pl.ds(me * heads, heads)], dst.at[b, :, slots, :], kv_own.at[kind, b])

    def half_cols(which):
        return pl.ds(pl.multiple_of(which * half, half), half)

    wo_send = remote(wo_ref.at[:, half_cols(1 - core)], wo_peer, wo_sems.at[0], wo_sems.at[1], partner)
    wo_send.start()
    for b in range(rows):
        for kind in range(2):
            for n in range(len(hops)):
                cache_copy(kind, b, n).start()

    for b in range(rows):
        for kind in range(2):
            own_copy(kind, b).start()
    wo_load = pltpu.make_async_copy(wo_ref.at[:, half_cols(core)], wo_own, in_sem.at[3])
    wo_load.start()
    zero_tail = jnp.zeros((rows, heads, steps, head_dim), BF16)
    kf[:, :, seq_len:, :] = zero_tail
    vf[:, :, seq_len:, :] = zero_tail

    def columns(which_core, which_chip):
        return pl.ds(pl.multiple_of(which_core * half + which_chip * block, block), block)

    loads = [
        pltpu.make_async_copy(gain_ref, gs, in_sem.at[0]),
        pltpu.make_async_copy(freq_ref, freq, in_sem.at[1]),
        pltpu.make_async_copy(plen_hbm, plen_ref, in_sem.at[2]),
    ]
    for c in loads:
        c.start()
    groups = width // head_dim
    w_loads = [
        pltpu.make_async_copy((wq_ref, wk_ref, wv_ref)[i // groups].at[:, i % groups * head_dim:(i % groups + 1) * head_dim], wb.at[i % 2], w_sem.at[i])
        for i in range(3 * groups)
    ]
    w_loads[0].start()
    w_loads[1].start()
    for c in loads:
        c.wait()

    part_steps = stage.shape[0]
    for t in range(0, steps, part_steps):
        x_load = pltpu.make_async_copy(x_ref.at[t:t + part_steps], stage, in_sem.at[4])
        x_load.start()
        x_load.wait()

        for b in range(rows):
            xs[b, t:t + part_steps, :] = stage[:, b, columns(core, chip)]
            squares = jnp.zeros((part_steps, block), F32)
            for c in range(0, model, block):
                residual = stage[:, b, c:c + block].astype(F32)
                squares = squares + residual * residual
            inv_rms = lax.rsqrt(jnp.sum(squares, axis=-1, keepdims=True) * (1.0 / model) + NORM_EPS)
            for c in range(0, model, block):
                residual = stage[:, b, c:c + block].astype(F32)
                gain = 1.0 + gs[c:c + block].astype(F32).reshape(1, block)
                hp[b * steps + t:b * steps + t + part_steps, c:c + block] = (residual * inv_rms * gain).astype(BF16)

    def lane_tile(n):
        return pl.ds(pl.multiple_of(n * head_dim, head_dim), head_dim)

    step_id = lax.broadcasted_iota(jnp.int32, (steps, head_dim), 0)
    for b in range(rows):
        angles = (step_id + plen_ref[b]).astype(F32) * freq[0:1, :]
        sc[:, b * head_dim:(b + 1) * head_dim] = jnp.cos(angles)
        sc[:, (rows + b) * head_dim:(rows + b + 1) * head_dim] = jnp.sin(angles) * freq[1:2, :]

    for i, load in enumerate(w_loads):
        load.wait()
        matrix, j = i // groups, i % groups

        @pl.loop(0, rows)
        def _(b, i=i, matrix=matrix, j=j):
            u = dot(hp[pl.ds(pl.multiple_of(b * steps, steps), steps), :model], wb[i % 2]).astype(BF16)
            if matrix < 2:
                u = u.astype(F32)
                u = u * sc[:, lane_tile(b)] + pltpu.roll(u, head_dim // 2, 1) * sc[:, lane_tile(rows + b)]
                if matrix == 0:
                    u = u * head_dim ** -0.5
            (qs, kn, vn)[matrix][b, j] = u.astype(BF16)

        if i + 2 < len(w_loads):
            w_loads[i + 2].start()

    wo_load.wait()
    wo_send.wait()
    causal = lax.broadcasted_iota(jnp.int32, (steps, steps), 1) <= lax.broadcasted_iota(jnp.int32, (steps, steps), 0)
    slot_id = lax.broadcasted_iota(jnp.int32, (steps, shard), 1)

    lanes = wb.shape[2]
    tiles = block // lanes

    def head_rows(h):
        return pl.ds(pl.multiple_of(h * steps, steps), steps)

    def partial_rows(b, which_chip, tile=0, count=1):
        first = ((b * chips + which_chip) * tiles + tile) * steps
        return pl.ds(pl.multiple_of(first, steps), count * steps)

    def rs_copy(b, d):
        to = lax.rem(chip + d, chips)
        return remote(wb.at[0, partial_rows(b, to, 0, tiles)], rs.at[b, d - 1], rs_send.at[b, d - 1], rs_recv.at[b, d - 1], to * CORES + core)

    def head_tile(b, h, count=1):
        return pl.ds(pl.multiple_of((b * heads + h) * steps, steps), count * steps)

    def o_copy(b):
        return remote(wb.at[1, head_tile(b, 0, heads)], o_peer.at[b], o_send.at[b], o_recv.at[b], partner)

    @pl.loop(0, rows)
    def _(b):
        own_copy(0, b).wait()
        for n in range(len(hops)):
            cache_copy(0, b, n).wait_recv()
        length = plen_ref[b]

        @pl.loop(0, heads)
        def _(h):
            q = qs[b, h]

            def score(s, peak):
                cols = pl.ds(pl.multiple_of(s * shard, shard), shard)
                scores = dot_t(q, kf[b, h, cols, :])
                scores = jnp.where(slot_id < length - s * shard, scores, -jnp.inf)
                sc[:, cols] = scores
                return jnp.maximum(peak, scores)

            peak = lax.fori_loop(0, parts, score, jnp.full((steps, shard), -jnp.inf, F32))
            fresh = jnp.where(causal, dot_t(q, kn[b, h]), -jnp.inf)
            row_peak = jnp.maximum(jnp.max(peak, axis=-1, keepdims=True), jnp.max(fresh, axis=-1, keepdims=True))

            def exponent(s, total):
                cols = pl.ds(pl.multiple_of(s * shard, shard), shard)
                e = jnp.exp(sc[:, cols] - row_peak)
                sc[:, cols] = e
                return total + e

            total = lax.fori_loop(0, parts, exponent, jnp.zeros((steps, shard), F32))
            fresh = jnp.exp(fresh - row_peak)
            inv = 1.0 / (jnp.sum(total, axis=-1, keepdims=True) + jnp.sum(fresh, axis=-1, keepdims=True))

            @pl.loop(0, parts)
            def _(s):
                cols = pl.ds(pl.multiple_of(s * shard, shard), shard)
                hp[head_rows(h), cols] = (sc[:, cols] * inv).astype(BF16)

            pn[h] = (fresh * inv).astype(BF16)

        own_copy(1, b).wait()
        for n in range(len(hops)):
            cache_copy(1, b, n).wait_recv()

        @pl.loop(0, heads)
        def _(h):
            out = dot(pn[h], vn[b, h])
            for s in range(parts):
                cols = slice(s * shard, (s + 1) * shard)
                out = out + dot(hp[head_rows(h), cols], vf[b, h, cols, :])
            wb[1, head_tile(b, h)] = out.astype(BF16)

        o_copy(b).start()
        o_copy(b).wait_recv()

        @pl.loop(0, chips)
        def _(j):
            cols = pl.ds(pl.multiple_of(j * block, block), block)
            own = jnp.concatenate([wb[1, head_tile(b, h)] for h in range(heads)], axis=1)
            other = jnp.concatenate([o_peer[b, h * steps:(h + 1) * steps] for h in range(heads)], axis=1)
            part = (dot(own, wo_own[:, cols]) + dot(other, wo_peer[:, cols])).astype(BF16)
            for tile in range(tiles):
                wb[0, partial_rows(b, j, tile)] = part[:, tile * lanes:(tile + 1) * lanes]

        for d in range(1, chips):
            rs_copy(b, d).start()

    def ag_copy(b, d):
        to = lax.rem(chip + d, chips)
        mine = yf.at[b, :, columns(core, chip)]
        return remote(mine, mine, ag_send.at[b, d - 1], ag_recv.at[b, d - 1], to * CORES + core)

    def d_copy(b):
        mine = yf.at[b, :, half_cols(core)]
        return remote(mine, mine, d_send.at[b], d_recv.at[b], partner)

    for b in range(rows):
        for d in range(1, chips):
            rs_copy(b, d).wait_recv()
        for tile in range(tiles):
            cols = slice(tile * lanes, (tile + 1) * lanes)
            attn = wb[0, partial_rows(b, chip, tile)].astype(F32)
            for d in range(1, chips):
                attn = attn + rs[b, d - 1, tile * steps:(tile + 1) * steps].astype(F32)
            out_cols = pl.ds(pl.multiple_of(core * half + chip * block + tile * lanes, lanes), lanes)
            yf[b, :, out_cols] = (xs[b, :, cols].astype(F32) + attn).astype(BF16)
        for d in range(1, chips):
            ag_copy(b, d).start()
    for b in range(rows):
        for d in range(1, chips):
            ag_copy(b, d).wait_recv()
        d_copy(b).start()
    for b in range(rows):
        d_copy(b).wait()
        o_copy(b).wait_send()
        for d in range(1, chips):
            rs_copy(b, d).wait_send()
            ag_copy(b, d).wait_send()
        for kind in range(2):
            for n in range(len(hops)):
                cache_copy(kind, b, n).wait_send()


def write_kernel(plen_hbm, kf, vf, kn, vn, yf, k_out, v_out, y_out, plen_ref, win, ys, big_sem, win_sem, y_sem, plen_sem):
    rows, heads, steps, head_dim = kn.shape
    out_len = kf.shape[2]
    span = win.shape[3]
    last = out_len - span

    def start_of(b):
        p = plen_ref[b]
        return pl.multiple_of(jnp.minimum(p - lax.rem(p, WINDOW_ALIGN), last), WINDOW_ALIGN)

    def big(kind, b):
        src, dst = ((kf, k_out), (vf, v_out))[kind]
        return pltpu.make_async_copy(src.at[b], dst.at[b], big_sem.at[kind, b])

    def small(kind, b):
        return pltpu.make_async_copy(win.at[kind, b], (k_out, v_out)[kind].at[b, :, pl.ds(start_of(b), span), :], win_sem.at[kind, b])

    for b in range(rows):
        for kind in range(2):
            big(kind, b).start()
    plen_copy = pltpu.make_async_copy(plen_hbm, plen_ref, plen_sem)
    plen_copy.start()
    for b in range(rows):
        ys[:, b, :] = yf[b]
    y_copy = pltpu.make_async_copy(ys, y_out, y_sem)
    y_copy.start()
    plen_copy.wait()
    row_id = lax.broadcasted_iota(jnp.int32, (span, steps), 0)
    col_id = lax.broadcasted_iota(jnp.int32, (span, steps), 1)
    pos = lax.broadcasted_iota(jnp.int32, (span, head_dim), 0)
    for b in range(rows):
        start = start_of(b)
        offset = plen_ref[b] - start
        select = (row_id == col_id + offset).astype(BF16)
        fresh = (pos >= offset) & (pos < offset + steps)
        for kind in range(2):
            old, new = ((kf, kn), (vf, vn))[kind]
            for h in range(heads):
                moved = dot(select, new[b, h])
                kept = old[b, h, pl.ds(start, span), :].astype(F32)
                win[kind, b, h] = jnp.where(fresh, moved, kept).astype(BF16)
    for b in range(rows):
        for kind in range(2):
            big(kind, b).wait()
            small(kind, b).start()
    y_copy.wait()
    for b in range(rows):
        for kind in range(2):
            small(kind, b).wait()


def solution(mesh):
    parts = mesh.shape["tp"]
    chips = parts // CORES

    def local_block(k_cache, v_cache, prompt_len, x_steps, w_norm, w_q, w_k, w_v, w_o):
        rows, _, shard, head_dim = k_cache.shape
        steps, _, model = x_steps.shape
        width = w_q.shape[1]
        heads = width // head_dim
        seq_len = shard * parts
        out_len = seq_len + steps
        half = model // CORES
        block = half // chips
        tiles = block // head_dim
        half_dim = head_dim // 2
        inv_freq = (ROPE_BASE ** (-2.0 * np.arange(half_dim) / head_dim)).astype(np.float32)
        sign = np.where(np.arange(head_dim) < half_dim, -1.0, 1.0).astype(np.float32)
        freq = np.zeros((8, head_dim), np.float32)
        freq[0], freq[1] = np.tile(inv_freq, 2), sign
        dma = pltpu.SemaphoreType.DMA
        plen = pltpu.with_memory_space_constraint(prompt_len, pltpu.HBM)
        peers = parts - 1
        kf, vf, kn, vn, yf = pl.pallas_call(
            functools.partial(exchange_kernel, chips, steps),
            out_shape=(
                pltpu.VMEM((rows, heads, out_len, head_dim), BF16),
                pltpu.VMEM((rows, heads, out_len, head_dim), BF16),
                pltpu.VMEM((rows, heads, steps, head_dim), BF16),
                pltpu.VMEM((rows, heads, steps, head_dim), BF16),
                pltpu.VMEM((rows, steps, model), BF16),
            ),
            in_specs=[ANY] * 10,
            out_specs=(VMEM,) * 5,
            scratch_shapes=[
                pltpu.SMEM((rows,), jnp.int32),
                pltpu.VMEM((8, head_dim), F32),
                pltpu.VMEM((STAGE_STEPS, rows, model), BF16),
                pltpu.VMEM((model,), BF16),
                pltpu.VMEM((max(rows, heads) * steps, max(model, seq_len)), BF16),
                pltpu.VMEM((2, model, head_dim), BF16),
                pltpu.VMEM((steps, seq_len), F32),
                pltpu.VMEM((heads, steps, steps), BF16),
                pltpu.VMEM((rows, steps, block), BF16),
                pltpu.VMEM((width, half), BF16),
                pltpu.VMEM((width, half), BF16),
                pltpu.VMEM((rows, heads, steps, head_dim), BF16),
                pltpu.VMEM((rows, heads * steps, head_dim), BF16),
                pltpu.VMEM((rows, chips - 1, tiles * steps, head_dim), BF16),
                dma((2, rows, peers)),
                dma((2, rows, peers)),
                dma((2, rows)),
                dma((3 * width // head_dim,)),
                dma((5,)),
                dma((2,)),
                dma((rows,)),
                dma((rows,)),
                dma((rows, chips - 1)),
                dma((rows, chips - 1)),
                dma((rows, chips - 1)),
                dma((rows, chips - 1)),
                dma((rows,)),
                dma((rows,)),
            ],
            compiler_params=pltpu.CompilerParams(collective_id=0, has_side_effects=True, vmem_limit_bytes=VMEM_LIMIT),
        )(plen, *(pltpu.with_memory_space_constraint(a, pltpu.HBM) for a in (k_cache, v_cache, x_steps, w_norm, w_q, w_k, w_v, w_o, jnp.asarray(freq))))
        span = steps + WINDOW_ALIGN
        k_out, v_out, y = pl.pallas_call(
            write_kernel,
            out_shape=(
                jax.ShapeDtypeStruct((rows, heads, out_len, head_dim), BF16),
                jax.ShapeDtypeStruct((rows, heads, out_len, head_dim), BF16),
                jax.ShapeDtypeStruct((steps, rows, model), BF16),
            ),
            in_specs=[ANY] + [VMEM] * 5,
            out_specs=(ANY,) * 3,
            scratch_shapes=[
                pltpu.SMEM((rows,), jnp.int32),
                pltpu.VMEM((2, rows, heads, span, head_dim), BF16),
                pltpu.VMEM((steps, rows, model), BF16),
                dma((2, rows)),
                dma((2, rows)),
                dma,
                dma,
            ],
            compiler_params=pltpu.CompilerParams(vmem_limit_bytes=6 << 20),
        )(plen, kf, vf, kn, vn, yf)
        return y, k_out, v_out

    cache_spec = P("dp", None, "tp", None)
    col_spec = P(None, "tp")
    out_cache_spec = P("dp", "tp", None, None)
    return jax.shard_map(local_block, mesh=mesh, in_specs=(cache_spec, cache_spec, P("dp"), P(None, "dp", None), P(None), col_spec, col_spec, col_spec, P("tp", None)), out_specs=(P(None, "dp", None), out_cache_spec, out_cache_spec), check_vma=False)
```

```python
import functools

import jax
import jax.numpy as jnp
import numpy as np
from jax import lax
from jax.experimental import pallas as pl
from jax.experimental.pallas import tpu as pltpu
from jax.sharding import PartitionSpec as P

ROPE_BASE = 10000.0
NORM_EPS = 1e-6
CORES = 2
WINDOW_ALIGN = 16
STAGE_STEPS = 8
VMEM_LIMIT = 12480 << 10
MESH = pl.DeviceIdType.MESH
F32 = jnp.float32
BF16 = jnp.bfloat16
ANY = pl.BlockSpec(memory_space=pl.ANY)
VMEM = pl.BlockSpec(memory_space=pltpu.VMEM)


def dot(a, b):
    return lax.dot_general(a, b, (((1,), (0,)), ((), ())), preferred_element_type=F32)


def dot_t(a, b):
    return lax.dot_general(a, b, (((1,), (1,)), ((), ())), preferred_element_type=F32)


def exchange_kernel(
    chips, steps, plen_hbm, k_ref, v_ref, x_ref, gain_ref, wq_ref, wk_ref, wv_ref, wo_ref, freq_ref,
    kf, vf, kn, vn, yf,
    plen_ref, freq, stage, gs, hp, wb, sc, pn, xs, wo_own, wo_peer, qs, o_peer, rs,
    kv_send, kv_recv, kv_own, w_sem, in_sem, wo_sems, o_send, o_recv, rs_send, rs_recv, ag_send, ag_recv, fw_send, fw_recv, d_send, d_recv,
):
    rows, heads, _, head_dim = kn.shape
    out_len = kf.shape[2]
    shard = k_ref.shape[2]
    seq_len = out_len - steps
    parts = chips * CORES
    model = wq_ref.shape[0]
    width = heads * head_dim
    half = model // CORES
    block = half // chips
    group = lax.axis_index("dp")
    me = lax.axis_index("tp")
    chip, core = me // CORES, lax.rem(me, CORES)
    partner = chip * CORES + (1 - core)

    hops = [(1, 0), (chips - 1, 0)] + [(d, 0) for d in range(2, chips - 1)]
    hops += [(1, 1), (chips - 1, 1)] + [(d, 1) for d in range(2, chips - 1)] + [(0, 1)]

    def peer(hop):
        return lax.rem(chip + hop[0], chips) * CORES + lax.rem(core + hop[1], CORES)

    def remote(src, dst, send, recv, target):
        return pltpu.make_async_remote_copy(src_ref=src, dst_ref=dst, send_sem=send, recv_sem=recv, device_id=(group, target), device_id_type=MESH)

    barrier = pltpu.get_barrier_semaphore()
    for hop in hops:
        pl.semaphore_signal(barrier, inc=1, device_id=(group, peer(hop)), device_id_type=MESH)
    pl.semaphore_wait(barrier, parts - 1)

    slots = pl.ds(pl.multiple_of(me * shard, shard), shard)

    def cache_copy(kind, b, n):
        src, dst = ((k_ref, kf), (v_ref, vf))[kind]
        target = peer(hops[n])
        return remote(src.at[b, pl.ds(target * heads, heads)], dst.at[b, :, slots, :], kv_send.at[kind, b, n], kv_recv.at[kind, b, n], target)

    def own_copy(kind, b):
        src, dst = ((k_ref, kf), (v_ref, vf))[kind]
        return pltpu.make_async_copy(src.at[b, pl.ds(me * heads, heads)], dst.at[b, :, slots, :], kv_own.at[kind, b])

    def half_cols(which):
        return pl.ds(pl.multiple_of(which * half, half), half)

    wo_send = remote(wo_ref.at[:, half_cols(1 - core)], wo_peer, wo_sems.at[0], wo_sems.at[1], partner)
    wo_send.start()
    for b in range(rows):
        for kind in range(2):
            for n in range(len(hops)):
                cache_copy(kind, b, n).start()

    for b in range(rows):
        for kind in range(2):
            own_copy(kind, b).start()
    wo_load = pltpu.make_async_copy(wo_ref.at[:, half_cols(core)], wo_own, in_sem.at[3])
    wo_load.start()
    zero_tail = jnp.zeros((rows, heads, steps, head_dim), BF16)
    kf[:, :, seq_len:, :] = zero_tail
    vf[:, :, seq_len:, :] = zero_tail

    def columns(which_core, which_chip):
        return pl.ds(pl.multiple_of(which_core * half + which_chip * block, block), block)

    loads = [
        pltpu.make_async_copy(gain_ref, gs, in_sem.at[0]),
        pltpu.make_async_copy(freq_ref, freq, in_sem.at[1]),
        pltpu.make_async_copy(plen_hbm, plen_ref, in_sem.at[2]),
    ]
    for c in loads:
        c.start()
    groups = width // head_dim
    w_loads = [
        pltpu.make_async_copy((wq_ref, wk_ref, wv_ref)[i // groups].at[:, i % groups * head_dim:(i % groups + 1) * head_dim], wb.at[i % 2], w_sem.at[i])
        for i in range(3 * groups)
    ]
    w_loads[0].start()
    w_loads[1].start()
    for c in loads:
        c.wait()

    part_steps = stage.shape[0]
    for t in range(0, steps, part_steps):
        x_load = pltpu.make_async_copy(x_ref.at[t:t + part_steps], stage, in_sem.at[4])
        x_load.start()
        x_load.wait()

        for b in range(rows):
            xs[b, t:t + part_steps, :] = stage[:, b, columns(core, chip)]
            squares = jnp.zeros((part_steps, block), F32)
            for c in range(0, model, block):
                residual = stage[:, b, c:c + block].astype(F32)
                squares = squares + residual * residual
            inv_rms = lax.rsqrt(jnp.sum(squares, axis=-1, keepdims=True) * (1.0 / model) + NORM_EPS)
            for c in range(0, model, block):
                residual = stage[:, b, c:c + block].astype(F32)
                gain = 1.0 + gs[c:c + block].astype(F32).reshape(1, block)
                hp[b * steps + t:b * steps + t + part_steps, c:c + block] = (residual * inv_rms * gain).astype(BF16)

    def lane_tile(n):
        return pl.ds(pl.multiple_of(n * head_dim, head_dim), head_dim)

    step_id = lax.broadcasted_iota(jnp.int32, (steps, head_dim), 0)
    for b in range(rows):
        angles = (step_id + plen_ref[b]).astype(F32) * freq[0:1, :]
        sc[:, b * head_dim:(b + 1) * head_dim] = jnp.cos(angles)
        sc[:, (rows + b) * head_dim:(rows + b + 1) * head_dim] = jnp.sin(angles) * freq[1:2, :]

    for i, load in enumerate(w_loads):
        load.wait()
        matrix, j = i // groups, i % groups

        @pl.loop(0, rows)
        def _(b, i=i, matrix=matrix, j=j):
            u = dot(hp[pl.ds(pl.multiple_of(b * steps, steps), steps), :model], wb[i % 2]).astype(BF16)
            if matrix < 2:
                u = u.astype(F32)
                u = u * sc[:, lane_tile(b)] + pltpu.roll(u, head_dim // 2, 1) * sc[:, lane_tile(rows + b)]
                if matrix == 0:
                    u = u * head_dim ** -0.5
            (qs, kn, vn)[matrix][b, j] = u.astype(BF16)

        if i + 2 < len(w_loads):
            w_loads[i + 2].start()

    wo_load.wait()
    wo_send.wait()
    causal = lax.broadcasted_iota(jnp.int32, (steps, steps), 1) <= lax.broadcasted_iota(jnp.int32, (steps, steps), 0)
    slot_id = lax.broadcasted_iota(jnp.int32, (steps, shard), 1)

    lanes = wb.shape[2]
    tiles = block // lanes

    def head_rows(h):
        return pl.ds(pl.multiple_of(h * steps, steps), steps)

    def partial_rows(b, which_chip, tile=0, count=1):
        first = ((b * chips + which_chip) * tiles + tile) * steps
        return pl.ds(pl.multiple_of(first, steps), count * steps)

    def rs_copy(b, d):
        to = lax.rem(chip + d, chips)
        return remote(wb.at[0, partial_rows(b, to, 0, tiles)], rs.at[b, d - 1], rs_send.at[b, d - 1], rs_recv.at[b, d - 1], to * CORES + core)

    def head_tile(b, h, count=1):
        return pl.ds(pl.multiple_of((b * heads + h) * steps, steps), count * steps)

    def o_copy(b):
        return remote(wb.at[1, head_tile(b, 0, heads)], o_peer.at[b], o_send.at[b], o_recv.at[b], partner)

    @pl.loop(0, rows)
    def _(b):
        own_copy(0, b).wait()
        for n in range(len(hops)):
            cache_copy(0, b, n).wait_recv()
        length = plen_ref[b]

        @pl.loop(0, heads)
        def _(h):
            q = qs[b, h]

            def score(s, peak):
                cols = pl.ds(pl.multiple_of(s * shard, shard), shard)
                scores = dot_t(q, kf[b, h, cols, :])
                scores = jnp.where(slot_id < length - s * shard, scores, -jnp.inf)
                sc[:, cols] = scores
                return jnp.maximum(peak, scores)

            peak = lax.fori_loop(0, parts, score, jnp.full((steps, shard), -jnp.inf, F32))
            fresh = jnp.where(causal, dot_t(q, kn[b, h]), -jnp.inf)
            row_peak = jnp.maximum(jnp.max(peak, axis=-1, keepdims=True), jnp.max(fresh, axis=-1, keepdims=True))

            def exponent(s, total):
                cols = pl.ds(pl.multiple_of(s * shard, shard), shard)
                e = jnp.exp(sc[:, cols] - row_peak)
                sc[:, cols] = e
                return total + e

            total = lax.fori_loop(0, parts, exponent, jnp.zeros((steps, shard), F32))
            fresh = jnp.exp(fresh - row_peak)
            inv = 1.0 / (jnp.sum(total, axis=-1, keepdims=True) + jnp.sum(fresh, axis=-1, keepdims=True))

            @pl.loop(0, parts)
            def _(s):
                cols = pl.ds(pl.multiple_of(s * shard, shard), shard)
                hp[head_rows(h), cols] = (sc[:, cols] * inv).astype(BF16)

            pn[h] = (fresh * inv).astype(BF16)

        own_copy(1, b).wait()
        for n in range(len(hops)):
            cache_copy(1, b, n).wait_recv()

        @pl.loop(0, heads)
        def _(h):
            out = dot(pn[h], vn[b, h])
            for s in range(parts):
                cols = slice(s * shard, (s + 1) * shard)
                out = out + dot(hp[head_rows(h), cols], vf[b, h, cols, :])
            wb[1, head_tile(b, h)] = out.astype(BF16)

        o_copy(b).start()
        o_copy(b).wait_recv()

        @pl.loop(0, chips)
        def _(j):
            cols = pl.ds(pl.multiple_of(j * block, block), block)
            own = jnp.concatenate([wb[1, head_tile(b, h)] for h in range(heads)], axis=1)
            other = jnp.concatenate([o_peer[b, h * steps:(h + 1) * steps] for h in range(heads)], axis=1)
            part = (dot(own, wo_own[:, cols]) + dot(other, wo_peer[:, cols])).astype(BF16)
            for tile in range(tiles):
                wb[0, partial_rows(b, j, tile)] = part[:, tile * lanes:(tile + 1) * lanes]

        for d in range(1, chips):
            rs_copy(b, d).start()

    sides = (1, chips - 1)

    def ag_copy(b, side):
        mine = yf.at[b, :, columns(core, chip)]
        to = lax.rem(chip + sides[side], chips)
        return remote(mine, mine, ag_send.at[b, side], ag_recv.at[b, side], to * CORES + core)

    def pass_copy(b, side):
        owner = lax.rem(chip + sides[1 - side], chips)
        part = block // 2
        cols = pl.ds(pl.multiple_of(core * half + owner * block + side * part, part), part)
        to = lax.rem(chip + sides[side], chips)
        return remote(yf.at[b, :, cols], yf.at[b, :, cols], fw_send.at[b, side], fw_recv.at[b, side], to * CORES + core)

    def d_copy(b):
        mine = yf.at[b, :, half_cols(core)]
        return remote(mine, mine, d_send.at[b], d_recv.at[b], partner)

    for b in range(rows):
        for d in range(1, chips):
            rs_copy(b, d).wait_recv()
        for tile in range(tiles):
            cols = slice(tile * lanes, (tile + 1) * lanes)
            attn = wb[0, partial_rows(b, chip, tile)].astype(F32)
            for d in range(1, chips):
                attn = attn + rs[b, d - 1, tile * steps:(tile + 1) * steps].astype(F32)
            out_cols = pl.ds(pl.multiple_of(core * half + chip * block + tile * lanes, lanes), lanes)
            yf[b, :, out_cols] = (xs[b, :, cols].astype(F32) + attn).astype(BF16)
        for side in range(2):
            ag_copy(b, side).start()
    for b in range(rows):
        for side in range(2):
            ag_copy(b, side).wait_recv()
            pass_copy(b, side).start()
    for b in range(rows):
        for side in range(2):
            pass_copy(b, side).wait_recv()
        d_copy(b).start()
    for b in range(rows):
        d_copy(b).wait()
        o_copy(b).wait_send()
        for d in range(1, chips):
            rs_copy(b, d).wait_send()
        for side in range(2):
            ag_copy(b, side).wait_send()
            pass_copy(b, side).wait_send()
        for kind in range(2):
            for n in range(len(hops)):
                cache_copy(kind, b, n).wait_send()


def write_kernel(plen_hbm, kf, vf, kn, vn, yf, k_out, v_out, y_out, plen_ref, win, ys, big_sem, win_sem, y_sem, plen_sem):
    rows, heads, steps, head_dim = kn.shape
    out_len = kf.shape[2]
    span = win.shape[3]
    last = out_len - span

    def start_of(b):
        p = plen_ref[b]
        return pl.multiple_of(jnp.minimum(p - lax.rem(p, WINDOW_ALIGN), last), WINDOW_ALIGN)

    def big(kind, b):
        src, dst = ((kf, k_out), (vf, v_out))[kind]
        return pltpu.make_async_copy(src.at[b], dst.at[b], big_sem.at[kind, b])

    def small(kind, b):
        return pltpu.make_async_copy(win.at[kind, b], (k_out, v_out)[kind].at[b, :, pl.ds(start_of(b), span), :], win_sem.at[kind, b])

    for b in range(rows):
        for kind in range(2):
            big(kind, b).start()
    plen_copy = pltpu.make_async_copy(plen_hbm, plen_ref, plen_sem)
    plen_copy.start()
    for b in range(rows):
        ys[:, b, :] = yf[b]
    y_copy = pltpu.make_async_copy(ys, y_out, y_sem)
    y_copy.start()
    plen_copy.wait()
    row_id = lax.broadcasted_iota(jnp.int32, (span, steps), 0)
    col_id = lax.broadcasted_iota(jnp.int32, (span, steps), 1)
    pos = lax.broadcasted_iota(jnp.int32, (span, head_dim), 0)
    for b in range(rows):
        start = start_of(b)
        offset = plen_ref[b] - start
        select = (row_id == col_id + offset).astype(BF16)
        fresh = (pos >= offset) & (pos < offset + steps)
        for kind in range(2):
            old, new = ((kf, kn), (vf, vn))[kind]
            for h in range(heads):
                moved = dot(select, new[b, h])
                kept = old[b, h, pl.ds(start, span), :].astype(F32)
                win[kind, b, h] = jnp.where(fresh, moved, kept).astype(BF16)
    for b in range(rows):
        for kind in range(2):
            big(kind, b).wait()
            small(kind, b).start()
    y_copy.wait()
    for b in range(rows):
        for kind in range(2):
            small(kind, b).wait()


def solution(mesh):
    parts = mesh.shape["tp"]
    chips = parts // CORES
    assert chips == 4

    def local_block(k_cache, v_cache, prompt_len, x_steps, w_norm, w_q, w_k, w_v, w_o):
        rows, _, shard, head_dim = k_cache.shape
        steps, _, model = x_steps.shape
        width = w_q.shape[1]
        heads = width // head_dim
        seq_len = shard * parts
        out_len = seq_len + steps
        half = model // CORES
        block = half // chips
        tiles = block // head_dim
        half_dim = head_dim // 2
        inv_freq = (ROPE_BASE ** (-2.0 * np.arange(half_dim) / head_dim)).astype(np.float32)
        sign = np.where(np.arange(head_dim) < half_dim, -1.0, 1.0).astype(np.float32)
        freq = np.zeros((8, head_dim), np.float32)
        freq[0], freq[1] = np.tile(inv_freq, 2), sign
        dma = pltpu.SemaphoreType.DMA
        plen = pltpu.with_memory_space_constraint(prompt_len, pltpu.HBM)
        peers = parts - 1
        kf, vf, kn, vn, yf = pl.pallas_call(
            functools.partial(exchange_kernel, chips, steps),
            out_shape=(
                pltpu.VMEM((rows, heads, out_len, head_dim), BF16),
                pltpu.VMEM((rows, heads, out_len, head_dim), BF16),
                pltpu.VMEM((rows, heads, steps, head_dim), BF16),
                pltpu.VMEM((rows, heads, steps, head_dim), BF16),
                pltpu.VMEM((rows, steps, model), BF16),
            ),
            in_specs=[ANY] * 10,
            out_specs=(VMEM,) * 5,
            scratch_shapes=[
                pltpu.SMEM((rows,), jnp.int32),
                pltpu.VMEM((8, head_dim), F32),
                pltpu.VMEM((STAGE_STEPS, rows, model), BF16),
                pltpu.VMEM((model,), BF16),
                pltpu.VMEM((max(rows, heads) * steps, max(model, seq_len)), BF16),
                pltpu.VMEM((2, model, head_dim), BF16),
                pltpu.VMEM((steps, seq_len), F32),
                pltpu.VMEM((heads, steps, steps), BF16),
                pltpu.VMEM((rows, steps, block), BF16),
                pltpu.VMEM((width, half), BF16),
                pltpu.VMEM((width, half), BF16),
                pltpu.VMEM((rows, heads, steps, head_dim), BF16),
                pltpu.VMEM((rows, heads * steps, head_dim), BF16),
                pltpu.VMEM((rows, chips - 1, tiles * steps, head_dim), BF16),
                dma((2, rows, peers)),
                dma((2, rows, peers)),
                dma((2, rows)),
                dma((3 * width // head_dim,)),
                dma((5,)),
                dma((2,)),
                dma((rows,)),
                dma((rows,)),
                dma((rows, chips - 1)),
                dma((rows, chips - 1)),
                dma((rows, 2)),
                dma((rows, 2)),
                dma((rows, 2)),
                dma((rows, 2)),
                dma((rows,)),
                dma((rows,)),
            ],
            compiler_params=pltpu.CompilerParams(collective_id=0, has_side_effects=True, vmem_limit_bytes=VMEM_LIMIT),
        )(plen, *(pltpu.with_memory_space_constraint(a, pltpu.HBM) for a in (k_cache, v_cache, x_steps, w_norm, w_q, w_k, w_v, w_o, jnp.asarray(freq))))
        span = steps + WINDOW_ALIGN
        k_out, v_out, y = pl.pallas_call(
            write_kernel,
            out_shape=(
                jax.ShapeDtypeStruct((rows, heads, out_len, head_dim), BF16),
                jax.ShapeDtypeStruct((rows, heads, out_len, head_dim), BF16),
                jax.ShapeDtypeStruct((steps, rows, model), BF16),
            ),
            in_specs=[ANY] + [VMEM] * 5,
            out_specs=(ANY,) * 3,
            scratch_shapes=[
                pltpu.SMEM((rows,), jnp.int32),
                pltpu.VMEM((2, rows, heads, span, head_dim), BF16),
                pltpu.VMEM((steps, rows, model), BF16),
                dma((2, rows)),
                dma((2, rows)),
                dma,
                dma,
            ],
            compiler_params=pltpu.CompilerParams(vmem_limit_bytes=6 << 20),
        )(plen, kf, vf, kn, vn, yf)
        return y, k_out, v_out

    cache_spec = P("dp", None, "tp", None)
    col_spec = P(None, "tp")
    out_cache_spec = P("dp", "tp", None, None)
    return jax.shard_map(local_block, mesh=mesh, in_specs=(cache_spec, cache_spec, P("dp"), P(None, "dp", None), P(None), col_spec, col_spec, col_spec, P("tp", None)), out_specs=(P(None, "dp", None), out_cache_spec, out_cache_spec), check_vma=False)
```

```python
import functools

import jax
import jax.numpy as jnp
import numpy as np
from jax import lax
from jax.experimental import pallas as pl
from jax.experimental.pallas import tpu as pltpu
from jax.sharding import PartitionSpec as P

ROPE_BASE = 10000.0
NORM_EPS = 1e-6
CORES = 2
WINDOW_ALIGN = 16
STAGE_STEPS = 8
VMEM_LIMIT = 12480 << 10
MESH = pl.DeviceIdType.MESH
F32 = jnp.float32
BF16 = jnp.bfloat16
ANY = pl.BlockSpec(memory_space=pl.ANY)
VMEM = pl.BlockSpec(memory_space=pltpu.VMEM)


def dot(a, b):
    return lax.dot_general(a, b, (((1,), (0,)), ((), ())), preferred_element_type=F32)


def dot_t(a, b):
    return lax.dot_general(a, b, (((1,), (1,)), ((), ())), preferred_element_type=F32)


def exchange_kernel(
    chips, steps, plen_hbm, k_ref, v_ref, x_ref, gain_ref, wq_ref, wk_ref, wv_ref, wo_ref, freq_ref,
    kf, vf, kn, vn, yf,
    plen_ref, freq, stage, gs, hp, wb, sc, pn, xs, wo_own, wo_peer, qs, o_peer, rs,
    kv_send, kv_recv, kv_own, w_sem, in_sem, wo_sems, o_send, o_recv, rs_send, rs_recv, ag_send, ag_recv, fw_send, fw_recv, d_send, d_recv,
):
    rows, heads, _, head_dim = kn.shape
    out_len = kf.shape[2]
    shard = k_ref.shape[2]
    seq_len = out_len - steps
    parts = chips * CORES
    model = wq_ref.shape[0]
    width = heads * head_dim
    half = model // CORES
    block = half // chips
    group = lax.axis_index("dp")
    me = lax.axis_index("tp")
    chip, core = me // CORES, lax.rem(me, CORES)
    partner = chip * CORES + (1 - core)

    hops = [(1, 0), (chips - 1, 0)] + [(d, 0) for d in range(2, chips - 1)]
    hops += [(1, 1), (chips - 1, 1)] + [(d, 1) for d in range(2, chips - 1)] + [(0, 1)]

    def peer(hop):
        return lax.rem(chip + hop[0], chips) * CORES + lax.rem(core + hop[1], CORES)

    def remote(src, dst, send, recv, target):
        return pltpu.make_async_remote_copy(src_ref=src, dst_ref=dst, send_sem=send, recv_sem=recv, device_id=(group, target), device_id_type=MESH)

    barrier = pltpu.get_barrier_semaphore()
    for hop in hops:
        pl.semaphore_signal(barrier, inc=1, device_id=(group, peer(hop)), device_id_type=MESH)
    pl.semaphore_wait(barrier, parts - 1)

    slots = pl.ds(pl.multiple_of(me * shard, shard), shard)

    def cache_copy(kind, b, n):
        src, dst = ((k_ref, kf), (v_ref, vf))[kind]
        target = peer(hops[n])
        return remote(src.at[b, pl.ds(target * heads, heads)], dst.at[b, :, slots, :], kv_send.at[kind, b, n], kv_recv.at[kind, b, n], target)

    def own_copy(kind, b):
        src, dst = ((k_ref, kf), (v_ref, vf))[kind]
        return pltpu.make_async_copy(src.at[b, pl.ds(me * heads, heads)], dst.at[b, :, slots, :], kv_own.at[kind, b])

    def half_cols(which):
        return pl.ds(pl.multiple_of(which * half, half), half)

    wo_send = remote(wo_ref.at[:, half_cols(1 - core)], wo_peer, wo_sems.at[0], wo_sems.at[1], partner)
    wo_send.start()
    for b in range(rows):
        for kind in range(2):
            for n in range(len(hops)):
                cache_copy(kind, b, n).start()

    for b in range(rows):
        for kind in range(2):
            own_copy(kind, b).start()
    wo_load = pltpu.make_async_copy(wo_ref.at[:, half_cols(core)], wo_own, in_sem.at[3])
    wo_load.start()
    zero_tail = jnp.zeros((rows, heads, steps, head_dim), BF16)
    kf[:, :, seq_len:, :] = zero_tail
    vf[:, :, seq_len:, :] = zero_tail

    def columns(which_core, which_chip):
        return pl.ds(pl.multiple_of(which_core * half + which_chip * block, block), block)

    loads = [
        pltpu.make_async_copy(gain_ref, gs, in_sem.at[0]),
        pltpu.make_async_copy(freq_ref, freq, in_sem.at[1]),
        pltpu.make_async_copy(plen_hbm, plen_ref, in_sem.at[2]),
    ]
    for c in loads:
        c.start()
    groups = width // head_dim
    w_loads = [
        pltpu.make_async_copy((wq_ref, wk_ref, wv_ref)[i // groups].at[:, i % groups * head_dim:(i % groups + 1) * head_dim], wb.at[i % 2], w_sem.at[i])
        for i in range(3 * groups)
    ]
    w_loads[0].start()
    w_loads[1].start()
    for c in loads:
        c.wait()

    part_steps = stage.shape[0]
    for t in range(0, steps, part_steps):
        x_load = pltpu.make_async_copy(x_ref.at[t:t + part_steps], stage, in_sem.at[4])
        x_load.start()
        x_load.wait()

        for b in range(rows):
            xs[b, t:t + part_steps, :] = stage[:, b, columns(core, chip)]
            squares = jnp.zeros((part_steps, block), F32)
            for c in range(0, model, block):
                residual = stage[:, b, c:c + block].astype(F32)
                squares = squares + residual * residual
            inv_rms = lax.rsqrt(jnp.sum(squares, axis=-1, keepdims=True) * (1.0 / model) + NORM_EPS)
            for c in range(0, model, block):
                residual = stage[:, b, c:c + block].astype(F32)
                gain = 1.0 + gs[c:c + block].astype(F32).reshape(1, block)
                hp[b * steps + t:b * steps + t + part_steps, c:c + block] = (residual * inv_rms * gain).astype(BF16)

    def lane_tile(n):
        return pl.ds(pl.multiple_of(n * head_dim, head_dim), head_dim)

    step_id = lax.broadcasted_iota(jnp.int32, (steps, head_dim), 0)
    for b in range(rows):
        angles = (step_id + plen_ref[b]).astype(F32) * freq[0:1, :]
        sc[:, b * head_dim:(b + 1) * head_dim] = jnp.cos(angles)
        sc[:, (rows + b) * head_dim:(rows + b + 1) * head_dim] = jnp.sin(angles) * freq[1:2, :]

    for i, load in enumerate(w_loads):
        load.wait()
        matrix, j = i // groups, i % groups

        @pl.loop(0, rows)
        def _(b, i=i, matrix=matrix, j=j):
            u = dot(hp[pl.ds(pl.multiple_of(b * steps, steps), steps), :model], wb[i % 2]).astype(BF16)
            if matrix < 2:
                u = u.astype(F32)
                u = u * sc[:, lane_tile(b)] + pltpu.roll(u, head_dim // 2, 1) * sc[:, lane_tile(rows + b)]
                if matrix == 0:
                    u = u * head_dim ** -0.5
            (qs, kn, vn)[matrix][b, j] = u.astype(BF16)

        if i + 2 < len(w_loads):
            w_loads[i + 2].start()

    wo_load.wait()
    wo_send.wait()
    causal = lax.broadcasted_iota(jnp.int32, (steps, steps), 1) <= lax.broadcasted_iota(jnp.int32, (steps, steps), 0)
    slot_id = lax.broadcasted_iota(jnp.int32, (steps, shard), 1)

    lanes = wb.shape[2]
    tiles = block // lanes

    def head_rows(h):
        return pl.ds(pl.multiple_of(h * steps, steps), steps)

    def partial_rows(b, which_chip, tile=0, count=1):
        first = ((b * chips + which_chip) * tiles + tile) * steps
        return pl.ds(pl.multiple_of(first, steps), count * steps)

    def rs_copy(b, d):
        to = lax.rem(chip + d, chips)
        return remote(wb.at[0, partial_rows(b, to, 0, tiles)], rs.at[b, d - 1], rs_send.at[b, d - 1], rs_recv.at[b, d - 1], to * CORES + core)

    def head_tile(b, h, count=1):
        return pl.ds(pl.multiple_of((b * heads + h) * steps, steps), count * steps)

    def o_copy(b):
        return remote(wb.at[1, head_tile(b, 0, heads)], o_peer.at[b], o_send.at[b], o_recv.at[b], partner)

    @pl.loop(0, rows)
    def _(b):
        own_copy(0, b).wait()
        for n in range(len(hops)):
            cache_copy(0, b, n).wait_recv()
        length = plen_ref[b]

        @pl.loop(0, heads)
        def _(h):
            q = qs[b, h]

            def score(s, peak):
                cols = pl.ds(pl.multiple_of(s * shard, shard), shard)
                scores = dot_t(q, kf[b, h, cols, :])
                scores = jnp.where(slot_id < length - s * shard, scores, -jnp.inf)
                sc[:, cols] = scores
                return jnp.maximum(peak, scores)

            peak = lax.fori_loop(0, parts, score, jnp.full((steps, shard), -jnp.inf, F32))
            fresh = jnp.where(causal, dot_t(q, kn[b, h]), -jnp.inf)
            row_peak = jnp.maximum(jnp.max(peak, axis=-1, keepdims=True), jnp.max(fresh, axis=-1, keepdims=True))

            def exponent(s, total):
                cols = pl.ds(pl.multiple_of(s * shard, shard), shard)
                e = jnp.exp(sc[:, cols] - row_peak)
                sc[:, cols] = e
                return total + e

            total = lax.fori_loop(0, parts, exponent, jnp.zeros((steps, shard), F32))
            fresh = jnp.exp(fresh - row_peak)
            inv = 1.0 / (jnp.sum(total, axis=-1, keepdims=True) + jnp.sum(fresh, axis=-1, keepdims=True))

            @pl.loop(0, parts)
            def _(s):
                cols = pl.ds(pl.multiple_of(s * shard, shard), shard)
                hp[head_rows(h), cols] = (sc[:, cols] * inv).astype(BF16)

            pn[h] = (fresh * inv).astype(BF16)

        own_copy(1, b).wait()
        for n in range(len(hops)):
            cache_copy(1, b, n).wait_recv()

        @pl.loop(0, heads)
        def _(h):
            out = dot(pn[h], vn[b, h])
            for s in range(parts):
                cols = slice(s * shard, (s + 1) * shard)
                out = out + dot(hp[head_rows(h), cols], vf[b, h, cols, :])
            wb[1, head_tile(b, h)] = out.astype(BF16)

        o_copy(b).start()
        o_copy(b).wait_recv()

        @pl.loop(0, chips)
        def _(j):
            cols = pl.ds(pl.multiple_of(j * block, block), block)
            own = jnp.concatenate([wb[1, head_tile(b, h)] for h in range(heads)], axis=1)
            other = jnp.concatenate([o_peer[b, h * steps:(h + 1) * steps] for h in range(heads)], axis=1)
            part = (dot(own, wo_own[:, cols]) + dot(other, wo_peer[:, cols])).astype(BF16)
            for tile in range(tiles):
                wb[0, partial_rows(b, j, tile)] = part[:, tile * lanes:(tile + 1) * lanes]

        for d in range(1, chips):
            rs_copy(b, d).start()

    sides = (1, chips - 1)

    def ag_copy(b, side):
        mine = yf.at[b, :, columns(core, chip)]
        to = lax.rem(chip + sides[side], chips)
        return remote(mine, mine, ag_send.at[b, side], ag_recv.at[b, side], to * CORES + core)

    def pass_copy(b, side, flip=0):
        owner = lax.rem(chip + sides[1 - side], chips)
        part = block // 2
        cols = pl.ds(pl.multiple_of(core * half + owner * block + side * part, part), part)
        to = lax.rem(chip + sides[side], chips)
        n = b + flip
        target = to * CORES + lax.rem(core + flip, CORES)
        return remote(yf.at[b, :, cols], yf.at[b, :, cols], fw_send.at[n, side], fw_recv.at[n, side], target)

    def d_copy(b):
        mine = yf.at[b, :, half_cols(core)]
        return remote(mine, mine, d_send.at[b], d_recv.at[b], partner)

    last = rows - 1

    def d_block(n):
        mine = yf.at[last, :, columns(core, lax.rem(chip + (0, chips - 1, 1)[n], chips))]
        return remote(mine, mine, d_send.at[last + n], d_recv.at[last + n], partner)

    for b in range(rows):
        for d in range(1, chips):
            rs_copy(b, d).wait_recv()
        for tile in range(tiles):
            cols = slice(tile * lanes, (tile + 1) * lanes)
            attn = wb[0, partial_rows(b, chip, tile)].astype(F32)
            for d in range(1, chips):
                attn = attn + rs[b, d - 1, tile * steps:(tile + 1) * steps].astype(F32)
            out_cols = pl.ds(pl.multiple_of(core * half + chip * block + tile * lanes, lanes), lanes)
            yf[b, :, out_cols] = (xs[b, :, cols].astype(F32) + attn).astype(BF16)
        for side in range(2):
            ag_copy(b, side).start()
    d_block(0).start()
    for b in range(rows):
        for side in range(2):
            ag_copy(b, side).wait_recv()
            pass_copy(b, side).start()
            if b == last:
                pass_copy(b, side, 1).start()
                d_block(1 + side).start()
    for b in range(last):
        for side in range(2):
            pass_copy(b, side).wait_recv()
        d_copy(b).start()
    for b in range(last):
        d_copy(b).wait()
    for n in range(3):
        d_block(n).wait()
    for side in range(2):
        for flip in range(2):
            pass_copy(last, side, flip).wait()
    for b in range(rows):
        o_copy(b).wait_send()
        for d in range(1, chips):
            rs_copy(b, d).wait_send()
        for side in range(2):
            ag_copy(b, side).wait_send()
            if b < last:
                pass_copy(b, side).wait_send()
        for kind in range(2):
            for n in range(len(hops)):
                cache_copy(kind, b, n).wait_send()


def write_kernel(plen_hbm, kf, vf, kn, vn, yf, k_out, v_out, y_out, plen_ref, win, ys, big_sem, win_sem, y_sem, plen_sem):
    rows, heads, steps, head_dim = kn.shape
    out_len = kf.shape[2]
    span = win.shape[3]
    last = out_len - span

    def start_of(b):
        p = plen_ref[b]
        return pl.multiple_of(jnp.minimum(p - lax.rem(p, WINDOW_ALIGN), last), WINDOW_ALIGN)

    lower = (out_len - steps) // 2

    def big(kind, b, upper):
        src, dst = ((kf, k_out), (vf, v_out))[kind]
        part = slice(lower, out_len) if upper else slice(0, lower)
        return pltpu.make_async_copy(src.at[b, :, part], dst.at[b, :, part], big_sem.at[upper, kind, b])

    def small(kind, b):
        return pltpu.make_async_copy(win.at[kind, b], (k_out, v_out)[kind].at[b, :, pl.ds(start_of(b), span), :], win_sem.at[kind, b])

    for b in range(rows):
        for kind in range(2):
            big(kind, b, 1).start()
    for kind in range(2):
        big(kind, 0, 0).start()
    plen_copy = pltpu.make_async_copy(plen_hbm, plen_ref, plen_sem)
    plen_copy.start()
    for b in range(rows):
        ys[:, b, :] = yf[b]
    y_copy = pltpu.make_async_copy(ys, y_out, y_sem)
    y_copy.start()
    plen_copy.wait()
    row_id = lax.broadcasted_iota(jnp.int32, (span, steps), 0)
    col_id = lax.broadcasted_iota(jnp.int32, (span, steps), 1)
    pos = lax.broadcasted_iota(jnp.int32, (span, head_dim), 0)
    for b in range(rows):
        start = start_of(b)
        offset = plen_ref[b] - start
        select = (row_id == col_id + offset).astype(BF16)
        fresh = (pos >= offset) & (pos < offset + steps)
        for kind in range(2):
            old, new = ((kf, kn), (vf, vn))[kind]
            for h in range(heads):
                moved = dot(select, new[b, h])
                kept = old[b, h, pl.ds(start, span), :].astype(F32)
                win[kind, b, h] = jnp.where(fresh, moved, kept).astype(BF16)
    for b in range(rows):
        for kind in range(2):
            big(kind, b, 1).wait()
            small(kind, b).start()
            if b + 1 < rows:
                big(kind, b + 1, 0).start()
    y_copy.wait()
    for b in range(rows):
        for kind in range(2):
            big(kind, b, 0).wait()
            small(kind, b).wait()


def solution(mesh):
    parts = mesh.shape["tp"]
    chips = parts // CORES
    assert chips == 4

    def local_block(k_cache, v_cache, prompt_len, x_steps, w_norm, w_q, w_k, w_v, w_o):
        rows, _, shard, head_dim = k_cache.shape
        steps, _, model = x_steps.shape
        width = w_q.shape[1]
        heads = width // head_dim
        seq_len = shard * parts
        out_len = seq_len + steps
        half = model // CORES
        block = half // chips
        tiles = block // head_dim
        half_dim = head_dim // 2
        inv_freq = (ROPE_BASE ** (-2.0 * np.arange(half_dim) / head_dim)).astype(np.float32)
        sign = np.where(np.arange(head_dim) < half_dim, -1.0, 1.0).astype(np.float32)
        freq = np.zeros((8, head_dim), np.float32)
        freq[0], freq[1] = np.tile(inv_freq, 2), sign
        dma = pltpu.SemaphoreType.DMA
        plen = pltpu.with_memory_space_constraint(prompt_len, pltpu.HBM)
        peers = parts - 1
        kf, vf, kn, vn, yf = pl.pallas_call(
            functools.partial(exchange_kernel, chips, steps),
            out_shape=(
                pltpu.VMEM((rows, heads, out_len, head_dim), BF16),
                pltpu.VMEM((rows, heads, out_len, head_dim), BF16),
                pltpu.VMEM((rows, heads, steps, head_dim), BF16),
                pltpu.VMEM((rows, heads, steps, head_dim), BF16),
                pltpu.VMEM((rows, steps, model), BF16),
            ),
            in_specs=[ANY] * 10,
            out_specs=(VMEM,) * 5,
            scratch_shapes=[
                pltpu.SMEM((rows,), jnp.int32),
                pltpu.VMEM((8, head_dim), F32),
                pltpu.VMEM((STAGE_STEPS, rows, model), BF16),
                pltpu.VMEM((model,), BF16),
                pltpu.VMEM((max(rows, heads) * steps, max(model, seq_len)), BF16),
                pltpu.VMEM((2, model, head_dim), BF16),
                pltpu.VMEM((steps, seq_len), F32),
                pltpu.VMEM((heads, steps, steps), BF16),
                pltpu.VMEM((rows, steps, block), BF16),
                pltpu.VMEM((width, half), BF16),
                pltpu.VMEM((width, half), BF16),
                pltpu.VMEM((rows, heads, steps, head_dim), BF16),
                pltpu.VMEM((rows, heads * steps, head_dim), BF16),
                pltpu.VMEM((rows, chips - 1, tiles * steps, head_dim), BF16),
                dma((2, rows, peers)),
                dma((2, rows, peers)),
                dma((2, rows)),
                dma((3 * width // head_dim,)),
                dma((5,)),
                dma((2,)),
                dma((rows,)),
                dma((rows,)),
                dma((rows, chips - 1)),
                dma((rows, chips - 1)),
                dma((rows, 2)),
                dma((rows, 2)),
                dma((rows + 1, 2)),
                dma((rows + 1, 2)),
                dma((rows + 2,)),
                dma((rows + 2,)),
            ],
            compiler_params=pltpu.CompilerParams(collective_id=0, has_side_effects=True, vmem_limit_bytes=VMEM_LIMIT),
        )(plen, *(pltpu.with_memory_space_constraint(a, pltpu.HBM) for a in (k_cache, v_cache, x_steps, w_norm, w_q, w_k, w_v, w_o, jnp.asarray(freq))))
        span = steps + WINDOW_ALIGN
        k_out, v_out, y = pl.pallas_call(
            write_kernel,
            out_shape=(
                jax.ShapeDtypeStruct((rows, heads, out_len, head_dim), BF16),
                jax.ShapeDtypeStruct((rows, heads, out_len, head_dim), BF16),
                jax.ShapeDtypeStruct((steps, rows, model), BF16),
            ),
            in_specs=[ANY] + [VMEM] * 5,
            out_specs=(ANY,) * 3,
            scratch_shapes=[
                pltpu.SMEM((rows,), jnp.int32),
                pltpu.VMEM((2, rows, heads, span, head_dim), BF16),
                pltpu.VMEM((steps, rows, model), BF16),
                dma((2, 2, rows)),
                dma((2, rows)),
                dma,
                dma,
            ],
            compiler_params=pltpu.CompilerParams(vmem_limit_bytes=6 << 20),
        )(plen, kf, vf, kn, vn, yf)
        return y, k_out, v_out

    cache_spec = P("dp", None, "tp", None)
    col_spec = P(None, "tp")
    out_cache_spec = P("dp", "tp", None, None)
    return jax.shard_map(local_block, mesh=mesh, in_specs=(cache_spec, cache_spec, P("dp"), P(None, "dp", None), P(None), col_spec, col_spec, col_spec, P("tp", None)), out_specs=(P(None, "dp", None), out_cache_spec, out_cache_spec), check_vma=False)
```

```python
import functools

import jax
import jax.numpy as jnp
import numpy as np
from jax import lax
from jax.experimental import pallas as pl
from jax.experimental.pallas import tpu as pltpu
from jax.sharding import PartitionSpec as P

ROPE_BASE = 10000.0
NORM_EPS = 1e-6
CORES = 2
WINDOW_ALIGN = 16
STAGE_STEPS = 8
VMEM_LIMIT = 12480 << 10
MESH = pl.DeviceIdType.MESH
F32 = jnp.float32
BF16 = jnp.bfloat16
ANY = pl.BlockSpec(memory_space=pl.ANY)
VMEM = pl.BlockSpec(memory_space=pltpu.VMEM)


def dot(a, b):
    return lax.dot_general(a, b, (((1,), (0,)), ((), ())), preferred_element_type=F32)


def dot_t(a, b):
    return lax.dot_general(a, b, (((1,), (1,)), ((), ())), preferred_element_type=F32)


def exchange_kernel(
    chips, steps, plen_hbm, k_ref, v_ref, x_ref, gain_ref, wq_ref, wk_ref, wv_ref, wo_ref, freq_ref,
    kf, vf, kn, vn, yf,
    plen_ref, freq, stage, gs, hp, wb, sc, pn, xs, wo_own, wo_peer, qs, o_peer, rs,
    kv_send, kv_recv, kv_own, first_send, w_sem, in_sem, wo_sems, o_send, o_recv, rs_send, rs_recv, ag_send, ag_recv, fw_send, fw_recv, d_send, d_recv,
):
    rows, heads, _, head_dim = kn.shape
    out_len = kf.shape[2]
    shard = k_ref.shape[2]
    seq_len = out_len - steps
    parts = chips * CORES
    model = wq_ref.shape[0]
    width = heads * head_dim
    half = model // CORES
    block = half // chips
    group = lax.axis_index("dp")
    me = lax.axis_index("tp")
    chip, core = me // CORES, lax.rem(me, CORES)
    partner = chip * CORES + (1 - core)

    hops = [(1, 0), (chips - 1, 0)] + [(d, 0) for d in range(2, chips - 1)]
    hops += [(1, 1), (chips - 1, 1)] + [(d, 1) for d in range(2, chips - 1)] + [(0, 1)]

    def peer(hop):
        return lax.rem(chip + hop[0], chips) * CORES + lax.rem(core + hop[1], CORES)

    def remote(src, dst, send, recv, target):
        return pltpu.make_async_remote_copy(src_ref=src, dst_ref=dst, send_sem=send, recv_sem=recv, device_id=(group, target), device_id_type=MESH)

    def first_load(n):
        return pltpu.make_async_copy(k_ref.at[0, pl.ds(peer(hops[n]) * heads, heads), :steps], qs.at[n], in_sem.at[5 + n])

    for n in range(2):
        first_load(n).start()

    barrier = pltpu.get_barrier_semaphore()
    for hop in hops:
        pl.semaphore_signal(barrier, inc=1, device_id=(group, peer(hop)), device_id_type=MESH)
    pl.semaphore_wait(barrier, parts - 1)

    slots = pl.ds(pl.multiple_of(me * shard, shard), shard)

    def cache_copy(kind, b, n):
        src, dst = ((k_ref, kf), (v_ref, vf))[kind]
        target = peer(hops[n])
        skip = steps if kind == 0 and isinstance(b, int) and b == 0 and n < 2 else 0
        return remote(
            src.at[b, pl.ds(target * heads, heads), skip:],
            dst.at[b, :, pl.ds(pl.multiple_of(me * shard + skip, WINDOW_ALIGN), shard - skip), :],
            kv_send.at[kind, b, n],
            kv_recv.at[kind, b, n],
            target,
        )

    def first_copy(n):
        dst = kf.at[0, :, pl.ds(pl.multiple_of(me * shard, shard), steps), :]
        return remote(qs.at[n], dst, first_send.at[n], kv_recv.at[0, 0, n], peer(hops[n]))

    def own_copy(kind, b):
        src, dst = ((k_ref, kf), (v_ref, vf))[kind]
        return pltpu.make_async_copy(src.at[b, pl.ds(me * heads, heads)], dst.at[b, :, slots, :], kv_own.at[kind, b])

    def half_cols(which):
        return pl.ds(pl.multiple_of(which * half, half), half)

    wo_send = remote(wo_ref.at[:, half_cols(1 - core)], wo_peer, wo_sems.at[0], wo_sems.at[1], partner)
    for n in range(2):
        first_load(n).wait()
        first_copy(n).start()
    for n in range(2):
        cache_copy(0, 0, n).start()
    wo_send.start()
    for b in range(rows):
        for kind in range(2):
            for n in range(2 if b == kind == 0 else 0, len(hops)):
                cache_copy(kind, b, n).start()

    for b in range(rows):
        for kind in range(2):
            own_copy(kind, b).start()
    wo_load = pltpu.make_async_copy(wo_ref.at[:, half_cols(core)], wo_own, in_sem.at[3])
    wo_load.start()
    zero_tail = jnp.zeros((rows, heads, steps, head_dim), BF16)
    kf[:, :, seq_len:, :] = zero_tail
    vf[:, :, seq_len:, :] = zero_tail

    def columns(which_core, which_chip):
        return pl.ds(pl.multiple_of(which_core * half + which_chip * block, block), block)

    loads = [
        pltpu.make_async_copy(gain_ref, gs, in_sem.at[0]),
        pltpu.make_async_copy(freq_ref, freq, in_sem.at[1]),
        pltpu.make_async_copy(plen_hbm, plen_ref, in_sem.at[2]),
    ]
    for c in loads:
        c.start()
    groups = width // head_dim
    w_loads = [
        pltpu.make_async_copy((wq_ref, wk_ref, wv_ref)[i // groups].at[:, i % groups * head_dim:(i % groups + 1) * head_dim], wb.at[i % 2], w_sem.at[i])
        for i in range(3 * groups)
    ]
    w_loads[0].start()
    w_loads[1].start()
    for c in loads:
        c.wait()

    part_steps = stage.shape[0]
    for t in range(0, steps, part_steps):
        x_load = pltpu.make_async_copy(x_ref.at[t:t + part_steps], stage, in_sem.at[4])
        x_load.start()
        x_load.wait()

        for b in range(rows):
            xs[b, t:t + part_steps, :] = stage[:, b, columns(core, chip)]
            squares = jnp.zeros((part_steps, block), F32)
            for c in range(0, model, block):
                residual = stage[:, b, c:c + block].astype(F32)
                squares = squares + residual * residual
            inv_rms = lax.rsqrt(jnp.sum(squares, axis=-1, keepdims=True) * (1.0 / model) + NORM_EPS)
            for c in range(0, model, block):
                residual = stage[:, b, c:c + block].astype(F32)
                gain = 1.0 + gs[c:c + block].astype(F32).reshape(1, block)
                hp[b * steps + t:b * steps + t + part_steps, c:c + block] = (residual * inv_rms * gain).astype(BF16)

    def lane_tile(n):
        return pl.ds(pl.multiple_of(n * head_dim, head_dim), head_dim)

    step_id = lax.broadcasted_iota(jnp.int32, (steps, head_dim), 0)
    for b in range(rows):
        angles = (step_id + plen_ref[b]).astype(F32) * freq[0:1, :]
        sc[:, b * head_dim:(b + 1) * head_dim] = jnp.cos(angles)
        sc[:, (rows + b) * head_dim:(rows + b + 1) * head_dim] = jnp.sin(angles) * freq[1:2, :]

    for n in range(2):
        first_copy(n).wait_send()
    for i, load in enumerate(w_loads):
        load.wait()
        matrix, j = i // groups, i % groups

        @pl.loop(0, rows)
        def _(b, i=i, matrix=matrix, j=j):
            u = dot(hp[pl.ds(pl.multiple_of(b * steps, steps), steps), :model], wb[i % 2]).astype(BF16)
            if matrix < 2:
                u = u.astype(F32)
                u = u * sc[:, lane_tile(b)] + pltpu.roll(u, head_dim // 2, 1) * sc[:, lane_tile(rows + b)]
                if matrix == 0:
                    u = u * head_dim ** -0.5
            (qs, kn, vn)[matrix][b, j] = u.astype(BF16)

        if i + 2 < len(w_loads):
            w_loads[i + 2].start()

    wo_load.wait()
    wo_send.wait()
    causal = lax.broadcasted_iota(jnp.int32, (steps, steps), 1) <= lax.broadcasted_iota(jnp.int32, (steps, steps), 0)
    slot_id = lax.broadcasted_iota(jnp.int32, (steps, shard), 1)

    lanes = wb.shape[2]
    tiles = block // lanes

    def head_rows(h):
        return pl.ds(pl.multiple_of(h * steps, steps), steps)

    def partial_rows(b, which_chip, tile=0, count=1):
        first = ((b * chips + which_chip) * tiles + tile) * steps
        return pl.ds(pl.multiple_of(first, steps), count * steps)

    def rs_copy(b, d):
        to = lax.rem(chip + d, chips)
        return remote(wb.at[0, partial_rows(b, to, 0, tiles)], rs.at[b, d - 1], rs_send.at[b, d - 1], rs_recv.at[b, d - 1], to * CORES + core)

    def head_tile(b, h, count=1):
        return pl.ds(pl.multiple_of((b * heads + h) * steps, steps), count * steps)

    def o_copy(b):
        return remote(wb.at[1, head_tile(b, 0, heads)], o_peer.at[b], o_send.at[b], o_recv.at[b], partner)

    @pl.loop(0, rows)
    def _(b):
        own_copy(0, b).wait()
        for n in range(len(hops)):
            cache_copy(0, b, n).wait_recv()
        length = plen_ref[b]

        @pl.loop(0, heads)
        def _(h):
            q = qs[b, h]

            def score(s, peak):
                cols = pl.ds(pl.multiple_of(s * shard, shard), shard)
                scores = dot_t(q, kf[b, h, cols, :])
                scores = jnp.where(slot_id < length - s * shard, scores, -jnp.inf)
                sc[:, cols] = scores
                return jnp.maximum(peak, scores)

            peak = lax.fori_loop(0, parts, score, jnp.full((steps, shard), -jnp.inf, F32))
            fresh = jnp.where(causal, dot_t(q, kn[b, h]), -jnp.inf)
            row_peak = jnp.maximum(jnp.max(peak, axis=-1, keepdims=True), jnp.max(fresh, axis=-1, keepdims=True))

            def exponent(s, total):
                cols = pl.ds(pl.multiple_of(s * shard, shard), shard)
                e = jnp.exp(sc[:, cols] - row_peak)
                sc[:, cols] = e
                return total + e

            total = lax.fori_loop(0, parts, exponent, jnp.zeros((steps, shard), F32))
            fresh = jnp.exp(fresh - row_peak)
            inv = 1.0 / (jnp.sum(total, axis=-1, keepdims=True) + jnp.sum(fresh, axis=-1, keepdims=True))

            @pl.loop(0, parts)
            def _(s):
                cols = pl.ds(pl.multiple_of(s * shard, shard), shard)
                hp[head_rows(h), cols] = (sc[:, cols] * inv).astype(BF16)

            pn[h] = (fresh * inv).astype(BF16)

        own_copy(1, b).wait()
        for n in range(len(hops)):
            cache_copy(1, b, n).wait_recv()

        @pl.loop(0, heads)
        def _(h):
            out = dot(pn[h], vn[b, h])
            for s in range(parts):
                cols = slice(s * shard, (s + 1) * shard)
                out = out + dot(hp[head_rows(h), cols], vf[b, h, cols, :])
            wb[1, head_tile(b, h)] = out.astype(BF16)

        o_copy(b).start()
        o_copy(b).wait_recv()

        @pl.loop(0, chips)
        def _(j):
            cols = pl.ds(pl.multiple_of(j * block, block), block)
            own = jnp.concatenate([wb[1, head_tile(b, h)] for h in range(heads)], axis=1)
            other = jnp.concatenate([o_peer[b, h * steps:(h + 1) * steps] for h in range(heads)], axis=1)
            part = (dot(own, wo_own[:, cols]) + dot(other, wo_peer[:, cols])).astype(BF16)
            for tile in range(tiles):
                wb[0, partial_rows(b, j, tile)] = part[:, tile * lanes:(tile + 1) * lanes]

        for d in range(1, chips):
            rs_copy(b, d).start()

    sides = (1, chips - 1)

    def ag_copy(b, side):
        mine = yf.at[b, :, columns(core, chip)]
        to = lax.rem(chip + sides[side], chips)
        return remote(mine, mine, ag_send.at[b, side], ag_recv.at[b, side], to * CORES + core)

    def pass_copy(b, side, flip=0):
        owner = lax.rem(chip + sides[1 - side], chips)
        part = block // 2
        cols = pl.ds(pl.multiple_of(core * half + owner * block + side * part, part), part)
        to = lax.rem(chip + sides[side], chips)
        n = b + flip
        target = to * CORES + lax.rem(core + flip, CORES)
        return remote(yf.at[b, :, cols], yf.at[b, :, cols], fw_send.at[n, side], fw_recv.at[n, side], target)

    def d_copy(b):
        mine = yf.at[b, :, half_cols(core)]
        return remote(mine, mine, d_send.at[b], d_recv.at[b], partner)

    last = rows - 1

    def d_block(n):
        mine = yf.at[last, :, columns(core, lax.rem(chip + (0, chips - 1, 1)[n], chips))]
        return remote(mine, mine, d_send.at[last + n], d_recv.at[last + n], partner)

    for b in range(rows):
        for d in range(1, chips):
            rs_copy(b, d).wait_recv()
        for tile in range(tiles):
            cols = slice(tile * lanes, (tile + 1) * lanes)
            attn = wb[0, partial_rows(b, chip, tile)].astype(F32)
            for d in range(1, chips):
                attn = attn + rs[b, d - 1, tile * steps:(tile + 1) * steps].astype(F32)
            out_cols = pl.ds(pl.multiple_of(core * half + chip * block + tile * lanes, lanes), lanes)
            yf[b, :, out_cols] = (xs[b, :, cols].astype(F32) + attn).astype(BF16)
        for side in range(2):
            ag_copy(b, side).start()
    d_block(0).start()
    for b in range(rows):
        for side in range(2):
            ag_copy(b, side).wait_recv()
            pass_copy(b, side).start()
            if b == last:
                pass_copy(b, side, 1).start()
                d_block(1 + side).start()
    for b in range(last):
        for side in range(2):
            pass_copy(b, side).wait_recv()
        d_copy(b).start()
    for b in range(last):
        d_copy(b).wait()
    for n in range(3):
        d_block(n).wait()
    for side in range(2):
        for flip in range(2):
            pass_copy(last, side, flip).wait()
    for b in range(rows):
        o_copy(b).wait_send()
        for d in range(1, chips):
            rs_copy(b, d).wait_send()
        for side in range(2):
            ag_copy(b, side).wait_send()
            if b < last:
                pass_copy(b, side).wait_send()
        for kind in range(2):
            for n in range(len(hops)):
                cache_copy(kind, b, n).wait_send()


def write_kernel(plen_hbm, kf, vf, kn, vn, yf, k_out, v_out, y_out, plen_ref, win, ys, big_sem, win_sem, y_sem, plen_sem):
    rows, heads, steps, head_dim = kn.shape
    out_len = kf.shape[2]
    span = win.shape[3]
    last = out_len - span

    def start_of(b):
        p = plen_ref[b]
        return pl.multiple_of(jnp.minimum(p - lax.rem(p, WINDOW_ALIGN), last), WINDOW_ALIGN)

    lower = (out_len - steps) // 2

    def big(kind, b, upper):
        src, dst = ((kf, k_out), (vf, v_out))[kind]
        part = slice(lower, out_len) if upper else slice(0, lower)
        return pltpu.make_async_copy(src.at[b, :, part], dst.at[b, :, part], big_sem.at[upper, kind, b])

    def small(kind, b):
        return pltpu.make_async_copy(win.at[kind, b], (k_out, v_out)[kind].at[b, :, pl.ds(start_of(b), span), :], win_sem.at[kind, b])

    for b in range(rows):
        for kind in range(2):
            big(kind, b, 1).start()
    for kind in range(2):
        big(kind, 0, 0).start()
    plen_copy = pltpu.make_async_copy(plen_hbm, plen_ref, plen_sem)
    plen_copy.start()
    for b in range(rows):
        ys[:, b, :] = yf[b]
    y_copy = pltpu.make_async_copy(ys, y_out, y_sem)
    y_copy.start()
    plen_copy.wait()
    row_id = lax.broadcasted_iota(jnp.int32, (span, steps), 0)
    col_id = lax.broadcasted_iota(jnp.int32, (span, steps), 1)
    pos = lax.broadcasted_iota(jnp.int32, (span, head_dim), 0)
    for b in range(rows):
        start = start_of(b)
        offset = plen_ref[b] - start
        select = (row_id == col_id + offset).astype(BF16)
        fresh = (pos >= offset) & (pos < offset + steps)
        for kind in range(2):
            old, new = ((kf, kn), (vf, vn))[kind]
            for h in range(heads):
                moved = dot(select, new[b, h])
                kept = old[b, h, pl.ds(start, span), :].astype(F32)
                win[kind, b, h] = jnp.where(fresh, moved, kept).astype(BF16)
    for b in range(rows):
        for kind in range(2):
            big(kind, b, 1).wait()
            small(kind, b).start()
            if b + 1 < rows:
                big(kind, b + 1, 0).start()
    y_copy.wait()
    for b in range(rows):
        for kind in range(2):
            big(kind, b, 0).wait()
            small(kind, b).wait()


def solution(mesh):
    parts = mesh.shape["tp"]
    chips = parts // CORES
    assert chips == 4

    def local_block(k_cache, v_cache, prompt_len, x_steps, w_norm, w_q, w_k, w_v, w_o):
        rows, _, shard, head_dim = k_cache.shape
        steps, _, model = x_steps.shape
        width = w_q.shape[1]
        heads = width // head_dim
        seq_len = shard * parts
        out_len = seq_len + steps
        half = model // CORES
        block = half // chips
        tiles = block // head_dim
        half_dim = head_dim // 2
        inv_freq = (ROPE_BASE ** (-2.0 * np.arange(half_dim) / head_dim)).astype(np.float32)
        sign = np.where(np.arange(head_dim) < half_dim, -1.0, 1.0).astype(np.float32)
        freq = np.zeros((8, head_dim), np.float32)
        freq[0], freq[1] = np.tile(inv_freq, 2), sign
        dma = pltpu.SemaphoreType.DMA
        plen = pltpu.with_memory_space_constraint(prompt_len, pltpu.HBM)
        peers = parts - 1
        kf, vf, kn, vn, yf = pl.pallas_call(
            functools.partial(exchange_kernel, chips, steps),
            out_shape=(
                pltpu.VMEM((rows, heads, out_len, head_dim), BF16),
                pltpu.VMEM((rows, heads, out_len, head_dim), BF16),
                pltpu.VMEM((rows, heads, steps, head_dim), BF16),
                pltpu.VMEM((rows, heads, steps, head_dim), BF16),
                pltpu.VMEM((rows, steps, model), BF16),
            ),
            in_specs=[ANY] * 10,
            out_specs=(VMEM,) * 5,
            scratch_shapes=[
                pltpu.SMEM((rows,), jnp.int32),
                pltpu.VMEM((8, head_dim), F32),
                pltpu.VMEM((STAGE_STEPS, rows, model), BF16),
                pltpu.VMEM((model,), BF16),
                pltpu.VMEM((max(rows, heads) * steps, max(model, seq_len)), BF16),
                pltpu.VMEM((2, model, head_dim), BF16),
                pltpu.VMEM((steps, seq_len), F32),
                pltpu.VMEM((heads, steps, steps), BF16),
                pltpu.VMEM((rows, steps, block), BF16),
                pltpu.VMEM((width, half), BF16),
                pltpu.VMEM((width, half), BF16),
                pltpu.VMEM((rows, heads, steps, head_dim), BF16),
                pltpu.VMEM((rows, heads * steps, head_dim), BF16),
                pltpu.VMEM((rows, chips - 1, tiles * steps, head_dim), BF16),
                dma((2, rows, peers)),
                dma((2, rows, peers)),
                dma((2, rows)),
                dma((2,)),
                dma((3 * width // head_dim,)),
                dma((7,)),
                dma((2,)),
                dma((rows,)),
                dma((rows,)),
                dma((rows, chips - 1)),
                dma((rows, chips - 1)),
                dma((rows, 2)),
                dma((rows, 2)),
                dma((rows + 1, 2)),
                dma((rows + 1, 2)),
                dma((rows + 2,)),
                dma((rows + 2,)),
            ],
            compiler_params=pltpu.CompilerParams(collective_id=0, has_side_effects=True, vmem_limit_bytes=VMEM_LIMIT),
        )(plen, *(pltpu.with_memory_space_constraint(a, pltpu.HBM) for a in (k_cache, v_cache, x_steps, w_norm, w_q, w_k, w_v, w_o, jnp.asarray(freq))))
        span = steps + WINDOW_ALIGN
        k_out, v_out, y = pl.pallas_call(
            write_kernel,
            out_shape=(
                jax.ShapeDtypeStruct((rows, heads, out_len, head_dim), BF16),
                jax.ShapeDtypeStruct((rows, heads, out_len, head_dim), BF16),
                jax.ShapeDtypeStruct((steps, rows, model), BF16),
            ),
            in_specs=[ANY] + [VMEM] * 5,
            out_specs=(ANY,) * 3,
            scratch_shapes=[
                pltpu.SMEM((rows,), jnp.int32),
                pltpu.VMEM((2, rows, heads, span, head_dim), BF16),
                pltpu.VMEM((steps, rows, model), BF16),
                dma((2, 2, rows)),
                dma((2, rows)),
                dma,
                dma,
            ],
            compiler_params=pltpu.CompilerParams(vmem_limit_bytes=6 << 20),
        )(plen, kf, vf, kn, vn, yf)
        return y, k_out, v_out

    cache_spec = P("dp", None, "tp", None)
    col_spec = P(None, "tp")
    out_cache_spec = P("dp", "tp", None, None)
    return jax.shard_map(local_block, mesh=mesh, in_specs=(cache_spec, cache_spec, P("dp"), P(None, "dp", None), P(None), col_spec, col_spec, col_spec, P("tp", None)), out_specs=(P(None, "dp", None), out_cache_spec, out_cache_spec), check_vma=False)
```

```python
import functools

import jax
import jax.numpy as jnp
import numpy as np
from jax import lax
from jax.experimental import pallas as pl
from jax.experimental.pallas import tpu as pltpu
from jax.sharding import PartitionSpec as P

ROPE_BASE = 10000.0
NORM_EPS = 1e-6
CORES = 2
WINDOW_ALIGN = 16
STAGE_STEPS = 8
VMEM_LIMIT = 12480 << 10
MESH = pl.DeviceIdType.MESH
F32 = jnp.float32
BF16 = jnp.bfloat16
ANY = pl.BlockSpec(memory_space=pl.ANY)
VMEM = pl.BlockSpec(memory_space=pltpu.VMEM)


def dot(a, b):
    return lax.dot_general(a, b, (((1,), (0,)), ((), ())), preferred_element_type=F32)


def dot_t(a, b):
    return lax.dot_general(a, b, (((1,), (1,)), ((), ())), preferred_element_type=F32)


def exchange_kernel(
    chips, steps, plen_hbm, k_ref, v_ref, x_ref, gain_ref, wq_ref, wk_ref, wv_ref, wo_ref, freq_ref,
    kf, vf, kn, vn, yf,
    plen_ref, freq, stage, gs, hp, wb, sc, pn, xs, wo_own, wo_peer, qs, o_peer, rs,
    kv_send, kv_recv, kv_own, w_sem, in_sem, wo_sems, o_send, o_recv, rs_send, rs_recv, ag_send, ag_recv, fw_send, fw_recv, d_send, d_recv,
):
    rows, heads, _, head_dim = kn.shape
    out_len = kf.shape[2]
    shard = k_ref.shape[2]
    seq_len = out_len - steps
    parts = chips * CORES
    model = wq_ref.shape[0]
    width = heads * head_dim
    half = model // CORES
    block = half // chips
    group = lax.axis_index("dp")
    me = lax.axis_index("tp")
    chip, core = me // CORES, lax.rem(me, CORES)
    partner = chip * CORES + (1 - core)

    hops = [(1, 0), (chips - 1, 0)] + [(d, 0) for d in range(2, chips - 1)]
    hops += [(1, 1), (chips - 1, 1)] + [(d, 1) for d in range(2, chips - 1)] + [(0, 1)]

    def peer(hop):
        return lax.rem(chip + hop[0], chips) * CORES + lax.rem(core + hop[1], CORES)

    def remote(src, dst, send, recv, target):
        return pltpu.make_async_remote_copy(src_ref=src, dst_ref=dst, send_sem=send, recv_sem=recv, device_id=(group, target), device_id_type=MESH)

    barrier = pltpu.get_barrier_semaphore()
    for hop in hops:
        pl.semaphore_signal(barrier, inc=1, device_id=(group, peer(hop)), device_id_type=MESH)
    pl.semaphore_wait(barrier, parts - 1)

    slots = pl.ds(pl.multiple_of(me * shard, shard), shard)

    def cache_copy(kind, b, n):
        src, dst = ((k_ref, kf), (v_ref, vf))[kind]
        target = peer(hops[n])
        return remote(src.at[b, pl.ds(target * heads, heads)], dst.at[b, :, slots, :], kv_send.at[kind, b, n], kv_recv.at[kind, b, n], target)

    def own_copy(kind, b):
        src, dst = ((k_ref, kf), (v_ref, vf))[kind]
        return pltpu.make_async_copy(src.at[b, pl.ds(me * heads, heads)], dst.at[b, :, slots, :], kv_own.at[kind, b])

    def half_cols(which):
        return pl.ds(pl.multiple_of(which * half, half), half)

    wo_send = remote(wo_ref.at[:, half_cols(1 - core)], wo_peer, wo_sems.at[0], wo_sems.at[1], partner)
    wo_send.start()
    for b in range(rows):
        for kind in range(2):
            for n in range(len(hops)):
                cache_copy(kind, b, n).start()

    for b in range(rows):
        for kind in range(2):
            own_copy(kind, b).start()
    wo_load = pltpu.make_async_copy(wo_ref.at[:, half_cols(core)], wo_own, in_sem.at[3])
    wo_load.start()
    zero_tail = jnp.zeros((rows, heads, steps, head_dim), BF16)
    kf[:, :, seq_len:, :] = zero_tail
    vf[:, :, seq_len:, :] = zero_tail

    def columns(which_core, which_chip):
        return pl.ds(pl.multiple_of(which_core * half + which_chip * block, block), block)

    loads = [
        pltpu.make_async_copy(gain_ref, gs, in_sem.at[0]),
        pltpu.make_async_copy(freq_ref, freq, in_sem.at[1]),
        pltpu.make_async_copy(plen_hbm, plen_ref, in_sem.at[2]),
    ]
    for c in loads:
        c.start()
    groups = width // head_dim
    w_loads = [
        pltpu.make_async_copy((wq_ref, wk_ref, wv_ref)[i // groups].at[:, i % groups * head_dim:(i % groups + 1) * head_dim], wb.at[i % 2], w_sem.at[i])
        for i in range(3 * groups)
    ]
    w_loads[0].start()
    w_loads[1].start()
    for c in loads:
        c.wait()

    part_steps = stage.shape[0]
    for t in range(0, steps, part_steps):
        x_load = pltpu.make_async_copy(x_ref.at[t:t + part_steps], stage, in_sem.at[4])
        x_load.start()
        x_load.wait()

        for b in range(rows):
            xs[b, t:t + part_steps, :] = stage[:, b, columns(core, chip)]
            squares = jnp.zeros((part_steps, block), F32)
            for c in range(0, model, block):
                residual = stage[:, b, c:c + block].astype(F32)
                squares = squares + residual * residual
            inv_rms = lax.rsqrt(jnp.sum(squares, axis=-1, keepdims=True) * (1.0 / model) + NORM_EPS)
            for c in range(0, model, block):
                residual = stage[:, b, c:c + block].astype(F32)
                gain = 1.0 + gs[c:c + block].astype(F32).reshape(1, block)
                hp[b * steps + t:b * steps + t + part_steps, c:c + block] = (residual * inv_rms * gain).astype(BF16)

    def lane_tile(n):
        return pl.ds(pl.multiple_of(n * head_dim, head_dim), head_dim)

    step_id = lax.broadcasted_iota(jnp.int32, (steps, head_dim), 0)
    for b in range(rows):
        angles = (step_id + plen_ref[b]).astype(F32) * freq[0:1, :]
        sc[:, b * head_dim:(b + 1) * head_dim] = jnp.cos(angles)
        sc[:, (rows + b) * head_dim:(rows + b + 1) * head_dim] = jnp.sin(angles) * freq[1:2, :]

    for i, load in enumerate(w_loads):
        load.wait()
        matrix, j = i // groups, i % groups

        @pl.loop(0, rows)
        def _(b, i=i, matrix=matrix, j=j):
            u = dot(hp[pl.ds(pl.multiple_of(b * steps, steps), steps), :model], wb[i % 2]).astype(BF16)
            if matrix < 2:
                u = u.astype(F32)
                u = u * sc[:, lane_tile(b)] + pltpu.roll(u, head_dim // 2, 1) * sc[:, lane_tile(rows + b)]
                if matrix == 0:
                    u = u * head_dim ** -0.5
            (qs, kn, vn)[matrix][b, j] = u.astype(BF16)

        if i + 2 < len(w_loads):
            w_loads[i + 2].start()

    wo_load.wait()
    wo_send.wait()
    causal = lax.broadcasted_iota(jnp.int32, (steps, steps), 1) <= lax.broadcasted_iota(jnp.int32, (steps, steps), 0)
    slot_id = lax.broadcasted_iota(jnp.int32, (steps, shard), 1)

    lanes = wb.shape[2]
    tiles = block // lanes

    def head_rows(h):
        return pl.ds(pl.multiple_of(h * steps, steps), steps)

    def partial_rows(b, which_chip, tile=0, count=1):
        first = ((b * chips + which_chip) * tiles + tile) * steps
        return pl.ds(pl.multiple_of(first, steps), count * steps)

    def rs_copy(b, d):
        to = lax.rem(chip + d, chips)
        return remote(wb.at[0, partial_rows(b, to, 0, tiles)], rs.at[b, d - 1], rs_send.at[b, d - 1], rs_recv.at[b, d - 1], to * CORES + core)

    def head_tile(b, h, count=1):
        return pl.ds(pl.multiple_of((b * heads + h) * steps, steps), count * steps)

    def o_copy(b):
        return remote(wb.at[1, head_tile(b, 0, heads)], o_peer.at[b], o_send.at[b], o_recv.at[b], partner)

    @pl.loop(0, rows)
    def _(b):
        own_copy(0, b).wait()
        for n in range(len(hops)):
            cache_copy(0, b, n).wait_recv()
        length = plen_ref[b]

        @pl.loop(0, heads)
        def _(h):
            q = qs[b, h]

            def score(s, peak):
                cols = pl.ds(pl.multiple_of(s * shard, shard), shard)
                scores = dot_t(q, kf[b, h, cols, :])
                scores = jnp.where(slot_id < length - s * shard, scores, -jnp.inf)
                sc[:, cols] = scores
                return jnp.maximum(peak, scores)

            peak = lax.fori_loop(0, parts, score, jnp.full((steps, shard), -jnp.inf, F32))
            fresh = jnp.where(causal, dot_t(q, kn[b, h]), -jnp.inf)
            row_peak = jnp.maximum(jnp.max(peak, axis=-1, keepdims=True), jnp.max(fresh, axis=-1, keepdims=True))

            def exponent(s, total):
                cols = pl.ds(pl.multiple_of(s * shard, shard), shard)
                e = jnp.exp(sc[:, cols] - row_peak)
                sc[:, cols] = e
                return total + e

            total = lax.fori_loop(0, parts, exponent, jnp.zeros((steps, shard), F32))
            fresh = jnp.exp(fresh - row_peak)
            inv = 1.0 / (jnp.sum(total, axis=-1, keepdims=True) + jnp.sum(fresh, axis=-1, keepdims=True))

            @pl.loop(0, parts)
            def _(s):
                cols = pl.ds(pl.multiple_of(s * shard, shard), shard)
                hp[head_rows(h), cols] = (sc[:, cols] * inv).astype(BF16)

            pn[h] = (fresh * inv).astype(BF16)

        own_copy(1, b).wait()
        for n in range(len(hops)):
            cache_copy(1, b, n).wait_recv()

        @pl.loop(0, heads)
        def _(h):
            out = dot(pn[h], vn[b, h])
            for s in range(parts):
                cols = slice(s * shard, (s + 1) * shard)
                out = out + dot(hp[head_rows(h), cols], vf[b, h, cols, :])
            wb[1, head_tile(b, h)] = out.astype(BF16)

        o_copy(b).start()
        o_copy(b).wait_recv()

        @pl.loop(0, chips)
        def _(j):
            cols = pl.ds(pl.multiple_of(j * block, block), block)
            own = jnp.concatenate([wb[1, head_tile(b, h)] for h in range(heads)], axis=1)
            other = jnp.concatenate([o_peer[b, h * steps:(h + 1) * steps] for h in range(heads)], axis=1)
            part = (dot(own, wo_own[:, cols]) + dot(other, wo_peer[:, cols])).astype(BF16)
            for tile in range(tiles):
                wb[0, partial_rows(b, j, tile)] = part[:, tile * lanes:(tile + 1) * lanes]

        for d in range(1, chips):
            rs_copy(b, d).start()

    sides = (1, chips - 1)

    def ag_copy(b, side):
        mine = yf.at[b, :, columns(core, chip)]
        to = lax.rem(chip + sides[side], chips)
        return remote(mine, mine, ag_send.at[b, side], ag_recv.at[b, side], to * CORES + core)

    def pass_copy(b, side, flip=0):
        owner = lax.rem(chip + sides[1 - side], chips)
        part = block // 2
        cols = pl.ds(pl.multiple_of(core * half + owner * block + side * part, part), part)
        to = lax.rem(chip + sides[side], chips)
        n = b + flip
        target = to * CORES + lax.rem(core + flip, CORES)
        return remote(yf.at[b, :, cols], yf.at[b, :, cols], fw_send.at[n, side], fw_recv.at[n, side], target)

    def d_copy(b):
        mine = yf.at[b, :, half_cols(core)]
        return remote(mine, mine, d_send.at[b], d_recv.at[b], partner)

    last = rows - 1

    def d_block(n):
        mine = yf.at[last, :, columns(core, lax.rem(chip + (0, chips - 1, 1)[n], chips))]
        return remote(mine, mine, d_send.at[last + n], d_recv.at[last + n], partner)

    for b in range(rows):
        for d in range(1, chips):
            rs_copy(b, d).wait_recv()
        for tile in range(tiles):
            cols = slice(tile * lanes, (tile + 1) * lanes)
            attn = wb[0, partial_rows(b, chip, tile)].astype(F32)
            for d in range(1, chips):
                attn = attn + rs[b, d - 1, tile * steps:(tile + 1) * steps].astype(F32)
            out_cols = pl.ds(pl.multiple_of(core * half + chip * block + tile * lanes, lanes), lanes)
            yf[b, :, out_cols] = (xs[b, :, cols].astype(F32) + attn).astype(BF16)
        for side in range(2):
            ag_copy(b, side).start()
    d_block(0).start()
    for b in range(rows):
        for side in range(2):
            ag_copy(b, side).wait_recv()
            pass_copy(b, side).start()
            if b == last:
                pass_copy(b, side, 1).start()
                d_block(1 + side).start()
    for b in range(last):
        for side in range(2):
            pass_copy(b, side).wait_recv()
        d_copy(b).start()
    for b in range(last):
        d_copy(b).wait()
    for n in range(3):
        d_block(n).wait()
    for side in range(2):
        for flip in range(2):
            pass_copy(last, side, flip).wait()
    for b in range(rows):
        o_copy(b).wait_send()
        for d in range(1, chips):
            rs_copy(b, d).wait_send()
        for side in range(2):
            ag_copy(b, side).wait_send()
            if b < last:
                pass_copy(b, side).wait_send()
        for kind in range(2):
            for n in range(len(hops)):
                cache_copy(kind, b, n).wait_send()


def write_kernel(plen_hbm, kf, vf, kn, vn, yf, k_out, v_out, y_out, plen_ref, win, ys, big_sem, win_sem, y_sem, plen_sem):
    rows, heads, steps, head_dim = kn.shape
    out_len = kf.shape[2]
    span = win.shape[3]
    last = out_len - span

    def start_of(b):
        p = plen_ref[b]
        return pl.multiple_of(jnp.minimum(p - lax.rem(p, WINDOW_ALIGN), last), WINDOW_ALIGN)

    def big(kind, b, h):
        src, dst = ((kf, k_out), (vf, v_out))[kind]
        return pltpu.make_async_copy(src.at[b, h], dst.at[b, h], big_sem.at[kind, b, h])

    def small(kind, b):
        return pltpu.make_async_copy(win.at[kind, b], (k_out, v_out)[kind].at[b, :, pl.ds(start_of(b), span), :], win_sem.at[kind, b])

    for b in range(rows):
        for kind in range(2):
            for h in range(heads):
                big(kind, b, h).start()
    plen_copy = pltpu.make_async_copy(plen_hbm, plen_ref, plen_sem)
    plen_copy.start()
    for b in range(rows):
        ys[:, b, :] = yf[b]
    y_copy = pltpu.make_async_copy(ys, y_out, y_sem)
    y_copy.start()
    plen_copy.wait()
    row_id = lax.broadcasted_iota(jnp.int32, (span, steps), 0)
    col_id = lax.broadcasted_iota(jnp.int32, (span, steps), 1)
    pos = lax.broadcasted_iota(jnp.int32, (span, head_dim), 0)
    for b in range(rows):
        start = start_of(b)
        offset = plen_ref[b] - start
        select = (row_id == col_id + offset).astype(BF16)
        fresh = (pos >= offset) & (pos < offset + steps)
        for kind in range(2):
            old, new = ((kf, kn), (vf, vn))[kind]
            for h in range(heads):
                moved = dot(select, new[b, h])
                kept = old[b, h, pl.ds(start, span), :].astype(F32)
                win[kind, b, h] = jnp.where(fresh, moved, kept).astype(BF16)
    for b in range(rows):
        for kind in range(2):
            for h in range(heads):
                big(kind, b, h).wait()
            small(kind, b).start()
    y_copy.wait()
    for b in range(rows):
        for kind in range(2):
            small(kind, b).wait()


def solution(mesh):
    parts = mesh.shape["tp"]
    chips = parts // CORES
    assert chips == 4

    def local_block(k_cache, v_cache, prompt_len, x_steps, w_norm, w_q, w_k, w_v, w_o):
        rows, _, shard, head_dim = k_cache.shape
        steps, _, model = x_steps.shape
        width = w_q.shape[1]
        heads = width // head_dim
        seq_len = shard * parts
        out_len = seq_len + steps
        half = model // CORES
        block = half // chips
        tiles = block // head_dim
        half_dim = head_dim // 2
        inv_freq = (ROPE_BASE ** (-2.0 * np.arange(half_dim) / head_dim)).astype(np.float32)
        sign = np.where(np.arange(head_dim) < half_dim, -1.0, 1.0).astype(np.float32)
        freq = np.zeros((8, head_dim), np.float32)
        freq[0], freq[1] = np.tile(inv_freq, 2), sign
        dma = pltpu.SemaphoreType.DMA
        plen = pltpu.with_memory_space_constraint(prompt_len, pltpu.HBM)
        peers = parts - 1
        kf, vf, kn, vn, yf = pl.pallas_call(
            functools.partial(exchange_kernel, chips, steps),
            out_shape=(
                pltpu.VMEM((rows, heads, out_len, head_dim), BF16),
                pltpu.VMEM((rows, heads, out_len, head_dim), BF16),
                pltpu.VMEM((rows, heads, steps, head_dim), BF16),
                pltpu.VMEM((rows, heads, steps, head_dim), BF16),
                pltpu.VMEM((rows, steps, model), BF16),
            ),
            in_specs=[ANY] * 10,
            out_specs=(VMEM,) * 5,
            scratch_shapes=[
                pltpu.SMEM((rows,), jnp.int32),
                pltpu.VMEM((8, head_dim), F32),
                pltpu.VMEM((STAGE_STEPS, rows, model), BF16),
                pltpu.VMEM((model,), BF16),
                pltpu.VMEM((max(rows, heads) * steps, max(model, seq_len)), BF16),
                pltpu.VMEM((2, model, head_dim), BF16),
                pltpu.VMEM((steps, seq_len), F32),
                pltpu.VMEM((heads, steps, steps), BF16),
                pltpu.VMEM((rows, steps, block), BF16),
                pltpu.VMEM((width, half), BF16),
                pltpu.VMEM((width, half), BF16),
                pltpu.VMEM((rows, heads, steps, head_dim), BF16),
                pltpu.VMEM((rows, heads * steps, head_dim), BF16),
                pltpu.VMEM((rows, chips - 1, tiles * steps, head_dim), BF16),
                dma((2, rows, peers)),
                dma((2, rows, peers)),
                dma((2, rows)),
                dma((3 * width // head_dim,)),
                dma((5,)),
                dma((2,)),
                dma((rows,)),
                dma((rows,)),
                dma((rows, chips - 1)),
                dma((rows, chips - 1)),
                dma((rows, 2)),
                dma((rows, 2)),
                dma((rows + 1, 2)),
                dma((rows + 1, 2)),
                dma((rows + 2,)),
                dma((rows + 2,)),
            ],
            compiler_params=pltpu.CompilerParams(collective_id=0, has_side_effects=True, vmem_limit_bytes=VMEM_LIMIT),
        )(plen, *(pltpu.with_memory_space_constraint(a, pltpu.HBM) for a in (k_cache, v_cache, x_steps, w_norm, w_q, w_k, w_v, w_o, jnp.asarray(freq))))
        span = steps + WINDOW_ALIGN
        k_out, v_out, y = pl.pallas_call(
            write_kernel,
            out_shape=(
                jax.ShapeDtypeStruct((rows, heads, out_len, head_dim), BF16),
                jax.ShapeDtypeStruct((rows, heads, out_len, head_dim), BF16),
                jax.ShapeDtypeStruct((steps, rows, model), BF16),
            ),
            in_specs=[ANY] + [VMEM] * 5,
            out_specs=(ANY,) * 3,
            scratch_shapes=[
                pltpu.SMEM((rows,), jnp.int32),
                pltpu.VMEM((2, rows, heads, span, head_dim), BF16),
                pltpu.VMEM((steps, rows, model), BF16),
                dma((2, rows, heads)),
                dma((2, rows)),
                dma,
                dma,
            ],
            compiler_params=pltpu.CompilerParams(vmem_limit_bytes=6 << 20),
        )(plen, kf, vf, kn, vn, yf)
        return y, k_out, v_out

    cache_spec = P("dp", None, "tp", None)
    col_spec = P(None, "tp")
    out_cache_spec = P("dp", "tp", None, None)
    return jax.shard_map(local_block, mesh=mesh, in_specs=(cache_spec, cache_spec, P("dp"), P(None, "dp", None), P(None), col_spec, col_spec, col_spec, P("tp", None)), out_specs=(P(None, "dp", None), out_cache_spec, out_cache_spec), check_vma=False)
```

```python
import functools

import jax
import jax.numpy as jnp
import numpy as np
from jax import lax
from jax.experimental import pallas as pl
from jax.experimental.pallas import tpu as pltpu
from jax.sharding import PartitionSpec as P

ROPE_BASE = 10000.0
NORM_EPS = 1e-6
CORES = 2
WINDOW_ALIGN = 16
STAGE_STEPS = 8
VMEM_LIMIT = 12480 << 10
MESH = pl.DeviceIdType.MESH
F32 = jnp.float32
BF16 = jnp.bfloat16
ANY = pl.BlockSpec(memory_space=pl.ANY)
VMEM = pl.BlockSpec(memory_space=pltpu.VMEM)


def dot(a, b):
    return lax.dot_general(a, b, (((1,), (0,)), ((), ())), preferred_element_type=F32)


def dot_t(a, b):
    return lax.dot_general(a, b, (((1,), (1,)), ((), ())), preferred_element_type=F32)


def exchange_kernel(
    chips, steps, plen_hbm, k_ref, v_ref, x_ref, gain_ref, wq_ref, wk_ref, wv_ref, wo_ref, freq_ref,
    kf, vf, kn, vn, yf,
    plen_ref, freq, stage, gs, hp, wb, sc, pn, xs, wo_own, wo_peer, qs, o_peer, rs,
    kv_send, kv_recv, kv_own, w_sem, in_sem, wo_sems, o_send, o_recv, rs_send, rs_recv, ag_send, ag_recv, fw_send, fw_recv, d_send, d_recv,
):
    rows, heads, _, head_dim = kn.shape
    out_len = kf.shape[2]
    shard = k_ref.shape[2]
    seq_len = out_len - steps
    parts = chips * CORES
    model = wq_ref.shape[0]
    width = heads * head_dim
    half = model // CORES
    block = half // chips
    group = lax.axis_index("dp")
    me = lax.axis_index("tp")
    chip, core = me // CORES, lax.rem(me, CORES)
    partner = chip * CORES + (1 - core)

    hops = [(1, 0), (chips - 1, 0)] + [(d, 0) for d in range(2, chips - 1)]
    hops += [(1, 1), (chips - 1, 1)] + [(d, 1) for d in range(2, chips - 1)] + [(0, 1)]

    def peer(hop):
        return lax.rem(chip + hop[0], chips) * CORES + lax.rem(core + hop[1], CORES)

    def remote(src, dst, send, recv, target):
        return pltpu.make_async_remote_copy(src_ref=src, dst_ref=dst, send_sem=send, recv_sem=recv, device_id=(group, target), device_id_type=MESH)

    barrier = pltpu.get_barrier_semaphore()
    for hop in hops:
        pl.semaphore_signal(barrier, inc=1, device_id=(group, peer(hop)), device_id_type=MESH)
    pl.semaphore_wait(barrier, parts - 1)

    slots = pl.ds(pl.multiple_of(me * shard, shard), shard)

    def cache_copy(kind, b, n):
        src, dst = ((k_ref, kf), (v_ref, vf))[kind]
        target = peer(hops[n])
        return remote(src.at[b, pl.ds(target * heads, heads)], dst.at[b, :, slots, :], kv_send.at[kind, b, n], kv_recv.at[kind, b, n], target)

    def own_copy(kind, b):
        src, dst = ((k_ref, kf), (v_ref, vf))[kind]
        return pltpu.make_async_copy(src.at[b, pl.ds(me * heads, heads)], dst.at[b, :, slots, :], kv_own.at[kind, b])

    def half_cols(which):
        return pl.ds(pl.multiple_of(which * half, half), half)

    wo_send = remote(wo_ref.at[:, half_cols(1 - core)], wo_peer, wo_sems.at[0], wo_sems.at[1], partner)
    wo_send.start()
    for b in range(rows):
        for kind in range(2):
            for n in range(len(hops)):
                cache_copy(kind, b, n).start()

    for b in range(rows):
        for kind in range(2):
            own_copy(kind, b).start()
    wo_load = pltpu.make_async_copy(wo_ref.at[:, half_cols(core)], wo_own, in_sem.at[3])
    wo_load.start()
    zero_tail = jnp.zeros((rows, heads, steps, head_dim), BF16)
    kf[:, :, seq_len:, :] = zero_tail
    vf[:, :, seq_len:, :] = zero_tail

    def columns(which_core, which_chip):
        return pl.ds(pl.multiple_of(which_core * half + which_chip * block, block), block)

    loads = [
        pltpu.make_async_copy(gain_ref, gs, in_sem.at[0]),
        pltpu.make_async_copy(freq_ref, freq, in_sem.at[1]),
        pltpu.make_async_copy(plen_hbm, plen_ref, in_sem.at[2]),
    ]
    for c in loads:
        c.start()
    groups = width // head_dim
    w_loads = [
        pltpu.make_async_copy((wq_ref, wk_ref, wv_ref)[i // groups].at[:, i % groups * head_dim:(i % groups + 1) * head_dim], wb.at[i % 2], w_sem.at[i])
        for i in range(3 * groups)
    ]
    w_loads[0].start()
    w_loads[1].start()
    for c in loads:
        c.wait()

    part_steps = stage.shape[0]
    for t in range(0, steps, part_steps):
        x_load = pltpu.make_async_copy(x_ref.at[t:t + part_steps], stage, in_sem.at[4])
        x_load.start()
        x_load.wait()

        for b in range(rows):
            xs[b, t:t + part_steps, :] = stage[:, b, columns(core, chip)]
            squares = jnp.zeros((part_steps, block), F32)
            for c in range(0, model, block):
                residual = stage[:, b, c:c + block].astype(F32)
                squares = squares + residual * residual
            inv_rms = lax.rsqrt(jnp.sum(squares, axis=-1, keepdims=True) * (1.0 / model) + NORM_EPS)
            for c in range(0, model, block):
                residual = stage[:, b, c:c + block].astype(F32)
                gain = 1.0 + gs[c:c + block].astype(F32).reshape(1, block)
                hp[b * steps + t:b * steps + t + part_steps, c:c + block] = (residual * inv_rms * gain).astype(BF16)

    def lane_tile(n):
        return pl.ds(pl.multiple_of(n * head_dim, head_dim), head_dim)

    step_id = lax.broadcasted_iota(jnp.int32, (steps, head_dim), 0)
    for b in range(rows):
        angles = (step_id + plen_ref[b]).astype(F32) * freq[0:1, :]
        sc[:, b * head_dim:(b + 1) * head_dim] = jnp.cos(angles)
        sc[:, (rows + b) * head_dim:(rows + b + 1) * head_dim] = jnp.sin(angles) * freq[1:2, :]

    for i, load in enumerate(w_loads):
        load.wait()
        matrix, j = i // groups, i % groups

        @pl.loop(0, rows)
        def _(b, i=i, matrix=matrix, j=j):
            u = dot(hp[pl.ds(pl.multiple_of(b * steps, steps), steps), :model], wb[i % 2]).astype(BF16)
            if matrix < 2:
                u = u.astype(F32)
                u = u * sc[:, lane_tile(b)] + pltpu.roll(u, head_dim // 2, 1) * sc[:, lane_tile(rows + b)]
                if matrix == 0:
                    u = u * head_dim ** -0.5
            (qs, kn, vn)[matrix][b, j] = u.astype(BF16)

        if i + 2 < len(w_loads):
            w_loads[i + 2].start()

    wo_load.wait()
    wo_send.wait()
    causal = lax.broadcasted_iota(jnp.int32, (steps, steps), 1) <= lax.broadcasted_iota(jnp.int32, (steps, steps), 0)
    slot_id = lax.broadcasted_iota(jnp.int32, (steps, shard), 1)

    lanes = wb.shape[2]
    tiles = block // lanes

    def head_rows(h):
        return pl.ds(pl.multiple_of(h * steps, steps), steps)

    def partial_rows(b, which_chip, tile=0, count=1):
        first = ((b * chips + which_chip) * tiles + tile) * steps
        return pl.ds(pl.multiple_of(first, steps), count * steps)

    def rs_copy(b, d):
        to = lax.rem(chip + d, chips)
        return remote(wb.at[0, partial_rows(b, to, 0, tiles)], rs.at[b, d - 1], rs_send.at[b, d - 1], rs_recv.at[b, d - 1], to * CORES + core)

    def head_tile(b, h, count=1):
        return pl.ds(pl.multiple_of((b * heads + h) * steps, steps), count * steps)

    def o_copy(b):
        return remote(wb.at[1, head_tile(b, 0, heads)], o_peer.at[b], o_send.at[b], o_recv.at[b], partner)

    @pl.loop(0, rows)
    def _(b):
        own_copy(0, b).wait()
        for n in range(len(hops)):
            cache_copy(0, b, n).wait_recv()
        length = plen_ref[b]

        @pl.loop(0, heads)
        def _(h):
            q = qs[b, h]

            def score(s, peak):
                cols = pl.ds(pl.multiple_of(s * shard, shard), shard)
                scores = dot_t(q, kf[b, h, cols, :])
                scores = jnp.where(slot_id < length - s * shard, scores, -jnp.inf)
                sc[:, cols] = scores
                return jnp.maximum(peak, scores)

            peak = lax.fori_loop(0, parts, score, jnp.full((steps, shard), -jnp.inf, F32))
            fresh = jnp.where(causal, dot_t(q, kn[b, h]), -jnp.inf)
            row_peak = jnp.maximum(jnp.max(peak, axis=-1, keepdims=True), jnp.max(fresh, axis=-1, keepdims=True))

            def exponent(s, total):
                cols = pl.ds(pl.multiple_of(s * shard, shard), shard)
                e = jnp.exp(sc[:, cols] - row_peak)
                sc[:, cols] = e
                return total + e

            total = lax.fori_loop(0, parts, exponent, jnp.zeros((steps, shard), F32))
            fresh = jnp.exp(fresh - row_peak)
            inv = 1.0 / (jnp.sum(total, axis=-1, keepdims=True) + jnp.sum(fresh, axis=-1, keepdims=True))

            @pl.loop(0, parts)
            def _(s):
                cols = pl.ds(pl.multiple_of(s * shard, shard), shard)
                hp[head_rows(h), cols] = (sc[:, cols] * inv).astype(BF16)

            pn[h] = (fresh * inv).astype(BF16)

        own_copy(1, b).wait()
        for n in range(len(hops)):
            cache_copy(1, b, n).wait_recv()

        @pl.loop(0, heads)
        def _(h):
            out = dot(pn[h], vn[b, h])
            for s in range(parts):
                cols = slice(s * shard, (s + 1) * shard)
                out = out + dot(hp[head_rows(h), cols], vf[b, h, cols, :])
            wb[1, head_tile(b, h)] = out.astype(BF16)

        o_copy(b).start()
        o_copy(b).wait_recv()

        @pl.loop(0, chips)
        def _(j):
            cols = pl.ds(pl.multiple_of(j * block, block), block)
            own = jnp.concatenate([wb[1, head_tile(b, h)] for h in range(heads)], axis=1)
            other = jnp.concatenate([o_peer[b, h * steps:(h + 1) * steps] for h in range(heads)], axis=1)
            part = (dot(own, wo_own[:, cols]) + dot(other, wo_peer[:, cols])).astype(BF16)
            for tile in range(tiles):
                wb[0, partial_rows(b, j, tile)] = part[:, tile * lanes:(tile + 1) * lanes]

        for d in range(1, chips):
            rs_copy(b, d).start()

    sides = (1, chips - 1)

    def ag_copy(b, side):
        mine = yf.at[b, :, columns(core, chip)]
        to = lax.rem(chip + sides[side], chips)
        return remote(mine, mine, ag_send.at[b, side], ag_recv.at[b, side], to * CORES + core)

    def pass_copy(b, side, flip=0):
        owner = lax.rem(chip + sides[1 - side], chips)
        part = block // 2
        cols = pl.ds(pl.multiple_of(core * half + owner * block + side * part, part), part)
        to = lax.rem(chip + sides[side], chips)
        n = b + flip
        target = to * CORES + lax.rem(core + flip, CORES)
        return remote(yf.at[b, :, cols], yf.at[b, :, cols], fw_send.at[n, side], fw_recv.at[n, side], target)

    def d_copy(b):
        mine = yf.at[b, :, half_cols(core)]
        return remote(mine, mine, d_send.at[b], d_recv.at[b], partner)

    last = rows - 1

    def d_block(n):
        mine = yf.at[last, :, columns(core, lax.rem(chip + (0, chips - 1, 1)[n], chips))]
        return remote(mine, mine, d_send.at[last + n], d_recv.at[last + n], partner)

    for b in range(rows):
        for d in range(1, chips):
            rs_copy(b, d).wait_recv()
        for tile in range(tiles):
            cols = slice(tile * lanes, (tile + 1) * lanes)
            attn = wb[0, partial_rows(b, chip, tile)].astype(F32)
            for d in range(1, chips):
                attn = attn + rs[b, d - 1, tile * steps:(tile + 1) * steps].astype(F32)
            out_cols = pl.ds(pl.multiple_of(core * half + chip * block + tile * lanes, lanes), lanes)
            yf[b, :, out_cols] = (xs[b, :, cols].astype(F32) + attn).astype(BF16)
        for side in range(2):
            ag_copy(b, side).start()
    d_block(0).start()
    for b in range(rows):
        for side in range(2):
            ag_copy(b, side).wait_recv()
            pass_copy(b, side).start()
            if b == last:
                pass_copy(b, side, 1).start()
                d_block(1 + side).start()
    for b in range(last):
        for side in range(2):
            pass_copy(b, side).wait_recv()
        d_copy(b).start()
    for b in range(last):
        d_copy(b).wait()
    for n in range(3):
        d_block(n).wait()
    for side in range(2):
        for flip in range(2):
            pass_copy(last, side, flip).wait()
    for b in range(rows):
        o_copy(b).wait_send()
        for d in range(1, chips):
            rs_copy(b, d).wait_send()
        for side in range(2):
            ag_copy(b, side).wait_send()
            if b < last:
                pass_copy(b, side).wait_send()
        for kind in range(2):
            for n in range(len(hops)):
                cache_copy(kind, b, n).wait_send()


def write_kernel(plen_hbm, kf, vf, kn, vn, yf, k_out, v_out, y_out, plen_ref, win, ys, big_sem, win_sem, y_sem, plen_sem):
    rows, heads, steps, head_dim = kn.shape
    out_len = kf.shape[2]
    span = win.shape[3]
    last = out_len - span

    def start_of(b):
        p = plen_ref[b]
        return pl.multiple_of(jnp.minimum(p - lax.rem(p, WINDOW_ALIGN), last), WINDOW_ALIGN)

    def big(kind, b):
        src, dst = ((kf, k_out), (vf, v_out))[kind]
        return pltpu.make_async_copy(src.at[b], dst.at[b], big_sem.at[kind, b])

    def small(kind, b):
        return pltpu.make_async_copy(win.at[kind, b], (k_out, v_out)[kind].at[b, :, pl.ds(start_of(b), span), :], win_sem.at[kind, b])

    for b in range(rows):
        for kind in range(2):
            big(kind, b).start()
    plen_copy = pltpu.make_async_copy(plen_hbm, plen_ref, plen_sem)
    plen_copy.start()
    for b in range(rows):
        ys[:, b, :] = yf[b]
    y_copy = pltpu.make_async_copy(ys, y_out, y_sem)
    y_copy.start()
    plen_copy.wait()
    row_id = lax.broadcasted_iota(jnp.int32, (span, steps), 0)
    col_id = lax.broadcasted_iota(jnp.int32, (span, steps), 1)
    pos = lax.broadcasted_iota(jnp.int32, (span, head_dim), 0)
    for b in range(rows):
        start = start_of(b)
        offset = plen_ref[b] - start
        select = (row_id == col_id + offset).astype(BF16)
        fresh = (pos >= offset) & (pos < offset + steps)
        for kind in range(2):
            old, new = ((kf, kn), (vf, vn))[kind]
            for h in range(heads):
                moved = dot(select, new[b, h])
                kept = old[b, h, pl.ds(start, span), :].astype(F32)
                win[kind, b, h] = jnp.where(fresh, moved, kept).astype(BF16)
    for b in range(rows):
        for kind in range(2):
            big(kind, b).wait()
            small(kind, b).start()
    y_copy.wait()
    for b in range(rows):
        for kind in range(2):
            small(kind, b).wait()


def solution(mesh):
    parts = mesh.shape["tp"]
    chips = parts // CORES
    assert chips == 4

    def local_block(k_cache, v_cache, prompt_len, x_steps, w_norm, w_q, w_k, w_v, w_o):
        rows, _, shard, head_dim = k_cache.shape
        steps, _, model = x_steps.shape
        width = w_q.shape[1]
        heads = width // head_dim
        seq_len = shard * parts
        out_len = seq_len + steps
        half = model // CORES
        block = half // chips
        tiles = block // head_dim
        half_dim = head_dim // 2
        inv_freq = (ROPE_BASE ** (-2.0 * np.arange(half_dim) / head_dim)).astype(np.float32)
        sign = np.where(np.arange(head_dim) < half_dim, -1.0, 1.0).astype(np.float32)
        freq = np.zeros((8, head_dim), np.float32)
        freq[0], freq[1] = np.tile(inv_freq, 2), sign
        dma = pltpu.SemaphoreType.DMA
        plen = pltpu.with_memory_space_constraint(prompt_len, pltpu.HBM)
        peers = parts - 1
        kf, vf, kn, vn, yf = pl.pallas_call(
            functools.partial(exchange_kernel, chips, steps),
            out_shape=(
                pltpu.VMEM((rows, heads, out_len, head_dim), BF16),
                pltpu.VMEM((rows, heads, out_len, head_dim), BF16),
                pltpu.VMEM((rows, heads, steps, head_dim), BF16),
                pltpu.VMEM((rows, heads, steps, head_dim), BF16),
                pltpu.VMEM((rows, steps, model), BF16),
            ),
            in_specs=[ANY] * 10,
            out_specs=(VMEM,) * 5,
            scratch_shapes=[
                pltpu.SMEM((rows,), jnp.int32),
                pltpu.VMEM((8, head_dim), F32),
                pltpu.VMEM((STAGE_STEPS, rows, model), BF16),
                pltpu.VMEM((model,), BF16),
                pltpu.VMEM((max(rows, heads) * steps, max(model, seq_len)), BF16),
                pltpu.VMEM((2, model, head_dim), BF16),
                pltpu.VMEM((steps, seq_len), F32),
                pltpu.VMEM((heads, steps, steps), BF16),
                pltpu.VMEM((rows, steps, block), BF16),
                pltpu.VMEM((width, half), BF16),
                pltpu.VMEM((width, half), BF16),
                pltpu.VMEM((rows, heads, steps, head_dim), BF16),
                pltpu.VMEM((rows, heads * steps, head_dim), BF16),
                pltpu.VMEM((rows, chips - 1, tiles * steps, head_dim), BF16),
                dma((2, rows, peers)),
                dma((2, rows, peers)),
                dma((2, rows)),
                dma((3 * width // head_dim,)),
                dma((5,)),
                dma((2,)),
                dma((rows,)),
                dma((rows,)),
                dma((rows, chips - 1)),
                dma((rows, chips - 1)),
                dma((rows, 2)),
                dma((rows, 2)),
                dma((rows + 1, 2)),
                dma((rows + 1, 2)),
                dma((rows + 2,)),
                dma((rows + 2,)),
            ],
            compiler_params=pltpu.CompilerParams(collective_id=0, has_side_effects=True, vmem_limit_bytes=VMEM_LIMIT),
        )(plen, *(pltpu.with_memory_space_constraint(a, pltpu.HBM) for a in (k_cache, v_cache, x_steps, w_norm, w_q, w_k, w_v, w_o, jnp.asarray(freq))))
        span = steps + WINDOW_ALIGN
        k_out, v_out, y = pl.pallas_call(
            write_kernel,
            out_shape=(
                jax.ShapeDtypeStruct((rows, heads, out_len, head_dim), BF16),
                jax.ShapeDtypeStruct((rows, heads, out_len, head_dim), BF16),
                jax.ShapeDtypeStruct((steps, rows, model), BF16),
            ),
            in_specs=[ANY] + [VMEM] * 5,
            out_specs=(ANY,) * 3,
            scratch_shapes=[
                pltpu.SMEM((rows,), jnp.int32),
                pltpu.VMEM((2, rows, heads, span, head_dim), BF16),
                pltpu.VMEM((steps, rows, model), BF16),
                dma((2, rows)),
                dma((2, rows)),
                dma,
                dma,
            ],
            compiler_params=pltpu.CompilerParams(vmem_limit_bytes=6 << 20),
        )(plen, kf, vf, kn, vn, yf)
        return y, k_out, v_out

    cache_spec = P("dp", None, "tp", None)
    col_spec = P(None, "tp")
    out_cache_spec = P("dp", "tp", None, None)
    return jax.shard_map(local_block, mesh=mesh, in_specs=(cache_spec, cache_spec, P("dp"), P(None, "dp", None), P(None), col_spec, col_spec, col_spec, P("tp", None)), out_specs=(P(None, "dp", None), out_cache_spec, out_cache_spec), check_vma=False)
```
